256 devices in a mesh: groups: 2 (over y), patch: 16 (over z), cfg: 2 (over core), head: 4 (over x).
Axes of the slice: x: 4, y: 2, z: 16, core: 2. Of those that a mesh axis runs over, the one named last changes fastest.
The devices are a block of a 4x16x16 slice.
Arguments:
- img_hidden: bfloat16 [2, 8192, 3072], P('cfg', ('groups', 'patch')), parts along dimension 1, may hold values from -40 to 40
- txt_hidden: bfloat16 [2, 512, 3072], P('cfg', ('groups', 'patch')), parts along dimension 1, may hold values from -6 to 6
- modulation: float32 [4, 3, 3072], P(('groups', 'cfg')), parts along dimension 0, may hold values from -4 to 4
- w_qkv: bfloat16 [3072, 3, 1536], P(None, None, 'head'), may hold values from -0.109375 to 0.109375
- q_gain: float32 [128], replicated, may hold values from 1.2 to 2.5
- k_gain: float32 [128], replicated, may hold values from 1.2 to 2.5
- w_out: bfloat16 [1536, 3072], P('head'), may hold values from -0.15625 to 0.15625
- b_out: float32 [3072], replicated, may hold values from -3 to 3
- stale_kv: bfloat16 [2, 2, 8704, 1536], P('cfg', None, ('groups', 'patch'), 'head'), parts along dimension 2, may hold values from -500 to 500
- final_mod: float32 [4, 2, 3072], P(('groups', 'cfg')), parts along dimension 0, may hold values from -3 to 3
- w_final: bfloat16 [3072, 64], replicated, may hold values from -0.109375 to 0.109375
- b_final: float32 [64], replicated, may hold values from -3 to 3
- latent: float32 [8192, 64], P(('groups', 'patch', 'cfg', 'head')), parts along dimension 0, may hold values from -6 to 6
- prev_denoised: float32 [8192, 64], P(('groups', 'patch', 'cfg', 'head')), parts along dimension 0, may hold values from -24 to 24
- guidance: float32 [2], P('groups'), parts along dimension 0, may hold values from 2 to 5
- step_index: int32 [1], replicated, may hold values from 14 to 21
- step_count: int32 [1], replicated, may hold values from 24 to 27
Outputs:
- fresh_kv: bfloat16 [2, 2, 8704, 1536], P('cfg', None, ('groups', 'patch'), 'head'), parts along dimension 2
- next_latent: float32 [8192, 64], P(('groups', 'patch', 'cfg', 'head')), parts along dimension 0
- denoised: float32 [8192, 64], P(('groups', 'patch', 'cfg', 'head')), parts along dimension 0
The draws below stay inside these ranges and needn't reach their ends.
There are 2 independent parts, one for each index of `groups`. The reference program is written for one: setup_inputs(seed, part) draws one part's arguments, and reference() takes and returns one part's arrays. A program takes and returns all parts, laid end to end along the dimension named above; an argument that names none is the same for every part. Nothing has to cross between parts.
All inputs are finite; a program needn't handle non-finite values.
Results may differ from the reference program's by a relative error of at most 0.0075.
The reference program's roundings to bfloat16 on the way (of `weights`, `attn` and `final_in`) count: a program that leaves them out, or rounds other values in their place, can miss the bound.
Values may be sent and summed in bfloat16 or wider, within the bound.
A program may use at most 128 MiB of HBM per device.

```python
import math
import jax
import jax.numpy as jnp
from jax import lax

D = 3072
HD = 128
CH = 64
HEADS = 12
GRID_W = 128
IMG_DEV = 256
TXT_DEV = 16
IMG = 4096
TXT = 256
KV_DEV = 272
KVTOK = 4352
N_PATCH = 16


def draw_img_hidden(key, part):
    key_base = jax.random.fold_in(key, 0)
    values = jax.random.normal(key_base, (2, IMG, D), jnp.float32)
    return jnp.clip(values, -40.0, 40.0).astype(jnp.bfloat16)


def draw_stale_kv(key, part):
    key_base = jax.random.fold_in(key, 0)
    width = HEADS * HD
    values = jax.random.normal(key_base, (2, 2, KVTOK, width), jnp.float32)
    values = values * jnp.array([1.5, 1.0], jnp.float32).reshape(1, 2, 1, 1)
    return jnp.clip(values, -500.0, 500.0).astype(jnp.bfloat16)


def shard_levels(stream_key, shape, cuts, low, high):
    def one(axis_at, shards_of):
        steps = jax.random.uniform(jax.random.fold_in(jax.random.fold_in(stream_key, 6), axis_at), (shards_of,), jnp.float32, low / len(cuts), high / len(cuts))
        return jnp.repeat(jnp.exp(steps), shape[axis_at] // shards_of).reshape((-1,) + (1,) * (len(shape) - axis_at - 1))

    loudness = one(*cuts[0])
    for cut in cuts[1:]:
        loudness = loudness * one(*cut)
    return loudness


def normal_values(rng, extent, deviation, limit, shards=(), held_as=jnp.bfloat16):
    drawn = deviation * jax.random.normal(rng, extent, jnp.float32)
    if shards:
        drawn = drawn * shard_levels(rng, extent, shards, -0.22, 0.18)
    return jnp.clip(drawn, -limit, limit).astype(held_as)


def setup_inputs(seed: int = 0, part: int = 0) -> dict:
    splits = jax.random.split(jax.random.key(seed), 18)
    part_splits = jax.random.split(jax.random.fold_in(splits[17], part), 18)
    img_hidden = draw_img_hidden(jax.random.fold_in(jax.random.fold_in(splits[17], part), 71), part)
    txt_hidden = normal_values(part_splits[1], (2, TXT, D), 1.0, 6.0, ((0, 2), (1, 16)))
    modulation = normal_values(part_splits[2], (2, 3, D), 0.7, 4.0, ((0, 2),), jnp.float32)
    w_qkv = normal_values(splits[3], (D, 3, HEADS * HD), D ** -0.5, 0.109375, ((2, 4),))
    q_gain = jnp.clip(jnp.exp(jax.random.uniform(splits[4], (HD,), jnp.float32, math.log(1.2), math.log(2.5))), 1.2, 2.5)
    k_gain = jnp.clip(jnp.exp(jax.random.uniform(splits[5], (HD,), jnp.float32, math.log(1.2), math.log(2.5))), 1.2, 2.5)
    w_out = normal_values(splits[6], (HEADS * HD, D), (HEADS * HD) ** -0.5, 0.15625, ((0, 4),))
    b_out = normal_values(splits[7], (D,), 0.5, 3.0, (), jnp.float32)
    stale_kv = draw_stale_kv(jax.random.fold_in(jax.random.fold_in(splits[17], part), 71), part)
    final_mod = normal_values(part_splits[9], (2, 2, D), 0.5, 3.0, ((0, 2),), jnp.float32)
    w_final = normal_values(splits[10], (D, CH), D ** -0.5, 0.109375)
    b_final = normal_values(splits[11], (CH,), 0.5, 3.0, (), jnp.float32)
    latent = normal_values(part_splits[12], (IMG, CH), 1.0, 6.0, ((0, 128),), jnp.float32)
    prev_denoised = normal_values(part_splits[13], (IMG, CH), 4.0, 24.0, ((0, 128),), jnp.float32)
    guidance = jnp.clip(jax.random.uniform(part_splits[14], (1,), jnp.float32, 2.0, 5.0), 2.0, 5.0)
    step_index = jax.random.randint(splits[15], (1,), 14, 22).astype(jnp.int32)
    step_count = jax.random.randint(splits[16], (1,), 24, 28).astype(jnp.int32)
    return dict(img_hidden=img_hidden, txt_hidden=txt_hidden, modulation=modulation, w_qkv=w_qkv, q_gain=q_gain, k_gain=k_gain, w_out=w_out, b_out=b_out, stale_kv=stale_kv, final_mod=final_mod, w_final=w_final, b_final=b_final, latent=latent, prev_denoised=prev_denoised, guidance=guidance, step_index=step_index, step_count=step_count)


epsilon = 1e-06
time_shift = 3.0

def layer_norm(values):
    mean_val = lax.optimization_barrier(jnp.mean(values, axis=-1, keepdims=True))
    centered = values - mean_val
    variance = lax.optimization_barrier(jnp.mean(centered * centered, axis=-1, keepdims=True))
    return centered * lax.rsqrt(variance + epsilon)

def rms_norm(values, gain_vec):
    return values * lax.rsqrt(lax.optimization_barrier(jnp.mean(values * values, axis=-1, keepdims=True)) + epsilon) * gain_vec

def rotate(values, positions, grid_width):
    quarter = values.shape[-1] // 4
    freqs = 10000.0 ** (-jnp.arange(quarter, dtype=jnp.float32) / quarter)
    row_pos = (positions // grid_width).astype(jnp.float32)
    col_pos = (positions % grid_width).astype(jnp.float32)
    angles = jnp.stack([row_pos[:, None] * freqs[None, :], col_pos[:, None] * freqs[None, :]], axis=1)
    cosine = jnp.cos(angles)[:, None]
    sine = jnp.sin(angles)[:, None]
    shaped = values.reshape(values.shape[0], values.shape[1], 2, 2, quarter)
    first = shaped[:, :, :, 0]
    second = shaped[:, :, :, 1]
    turned = jnp.stack([first * cosine - second * sine, second * cosine + first * sine], axis=3)
    return turned.reshape(values.shape)

def noise_level(index, count):
    frac = 1.0 - index / count
    lift = math.exp(time_shift)
    return lift * frac / (lift * frac + 1.0 - frac)

def log_ratio(sigma_val):
    return jnp.log(1.0 - sigma_val) - jnp.log(sigma_val)

def solver_step(cond, uncond, guidance, step_index, step_count, latent, prev_denoised):
    guided = uncond + guidance[0] * (cond - uncond)
    index = step_index[0].astype(jnp.float32)
    count = step_count[0].astype(jnp.float32)
    sigma_prev = noise_level(index - 1.0, count)
    sigma_now = noise_level(index, count)
    sigma_next = noise_level(index + 1.0, count)
    step_now = log_ratio(sigma_next) - log_ratio(sigma_now)
    step_prev = log_ratio(sigma_now) - log_ratio(sigma_prev)
    ratio = step_prev / step_now
    denoised = latent - sigma_now * guided
    blend = (1.0 + 0.5 / ratio) * denoised - 0.5 / ratio * prev_denoised
    next_latent = sigma_next / sigma_now * latent - (1.0 - sigma_next) * (jnp.exp(-step_now) - 1.0) * blend
    return (next_latent, denoised)

def reference(img_hidden, txt_hidden, modulation, w_qkv, q_gain, k_gain, w_out, b_out, stale_kv, final_mod, w_final, b_final, latent, prev_denoised, guidance, step_index, step_count):
    inv_root = HD ** (-0.5)
    head_width = HEADS * HD
    weight_flat = w_qkv.reshape(D, 3 * head_width)
    positions = jnp.arange(IMG, dtype=jnp.int32)
    fresh_list = []
    velocities = []
    for branch in range(2):
        shift_vec = modulation[branch, 0]
        scale_vec = modulation[branch, 1]
        gate_vec = modulation[branch, 2]
        modded_img = (layer_norm(img_hidden[branch].astype(jnp.float32)) * (1.0 + scale_vec) + shift_vec).astype(jnp.bfloat16)
        modded_txt = (layer_norm(txt_hidden[branch].astype(jnp.float32)) * (1.0 + scale_vec) + shift_vec).astype(jnp.bfloat16)
        proj_img = jnp.dot(modded_img, weight_flat, preferred_element_type=jnp.float32).reshape(IMG, 3, HEADS, HD)
        proj_txt = jnp.dot(modded_txt, weight_flat, preferred_element_type=jnp.float32).reshape(TXT, 3, HEADS, HD)
        queries = lax.optimization_barrier(rotate(rms_norm(proj_img[:, 0], q_gain), positions, GRID_W).astype(jnp.bfloat16))
        img_keys = rotate(rms_norm(proj_img[:, 1], k_gain), positions, GRID_W).astype(jnp.bfloat16)
        img_vals = proj_img[:, 2].astype(jnp.bfloat16)
        txt_keys = rms_norm(proj_txt[:, 1], k_gain).astype(jnp.bfloat16)
        txt_vals = proj_txt[:, 2].astype(jnp.bfloat16)

        def joined(txt_part, img_part):
            return jnp.concatenate([txt_part.reshape(N_PATCH, TXT_DEV, HEADS, HD), img_part.reshape(N_PATCH, IMG_DEV, HEADS, HD)], axis=1).reshape(KVTOK, HEADS, HD)
        fresh_keys = lax.optimization_barrier(joined(txt_keys, img_keys))
        fresh_vals = lax.optimization_barrier(joined(txt_vals, img_vals))
        fresh_list.append(jnp.stack([fresh_keys.reshape(KVTOK, head_width), fresh_vals.reshape(KVTOK, head_width)]))
        stale_keys = stale_kv[branch, 0].reshape(KVTOK, HEADS, HD)
        stale_vals = stale_kv[branch, 1].reshape(KVTOK, HEADS, HD)

        def attend(block):
            query_blk = lax.dynamic_slice_in_dim(queries, block * IMG_DEV, IMG_DEV, 0)
            own_keys = lax.dynamic_slice_in_dim(fresh_keys, block * KV_DEV, KV_DEV, 0)
            own_vals = lax.dynamic_slice_in_dim(fresh_vals, block * KV_DEV, KV_DEV, 0)
            keys_all = lax.dynamic_update_slice_in_dim(stale_keys, own_keys, block * KV_DEV, 0)
            vals_all = lax.dynamic_update_slice_in_dim(stale_vals, own_vals, block * KV_DEV, 0)
            scores = jnp.einsum('qhd,khd->hqk', query_blk.astype(jnp.float32), keys_all.astype(jnp.float32)) * inv_root
            top = lax.optimization_barrier(jnp.max(scores, axis=-1, keepdims=True))
            expo = jnp.exp(scores - top)
            denom = lax.optimization_barrier(jnp.sum(expo, axis=-1))
            weights = lax.optimization_barrier(expo.astype(jnp.bfloat16))
            weighted = jnp.einsum('hqk,khd->hqd', weights.astype(jnp.float32), vals_all.astype(jnp.float32))
            attn_blk = weighted / denom[..., None]
            return attn_blk.transpose(1, 0, 2).reshape(IMG_DEV, head_width).astype(jnp.bfloat16)
        attn = lax.map(attend, jnp.arange(N_PATCH, dtype=jnp.int32)).reshape(IMG, head_width)
        projected = jnp.dot(attn, w_out, preferred_element_type=jnp.float32)
        mixed = img_hidden[branch].astype(jnp.float32) + gate_vec * (projected + b_out)
        final_in = (layer_norm(mixed) * (1.0 + final_mod[branch, 1]) + final_mod[branch, 0]).astype(jnp.bfloat16)
        velocities.append(jnp.dot(final_in, w_final, preferred_element_type=jnp.float32) + b_final)
    next_latent, denoised = solver_step(velocities[0], velocities[1], guidance, step_index, step_count, latent, prev_denoised)
    return (jnp.stack(fresh_list), next_latent, denoised)
```

```python
import functools
import math

import jax
import jax.numpy as jnp
import numpy as np
from jax import lax
from jax.experimental import pallas as pl
from jax.experimental.pallas import tpu as pltpu
from jax.sharding import PartitionSpec as P

HD = 128
GRID_W = 128
EPS = 1e-06
TIME_SHIFT = 3.0
MESH = pl.DeviceIdType.MESH
BF = jnp.bfloat16
F32 = jnp.float32


def rotation_tables(grid_rows):
    quarter = HD // 4
    freqs = 10000.0 ** (-np.arange(quarter, dtype=np.float32) / quarter)
    freqs = freqs.astype(np.float32)

    def half(count, at):
        angle = np.arange(count, dtype=np.float32)[:, None] * freqs[None, :]
        out = np.zeros((3, count, HD), np.float32)
        cosine = np.cos(angle.astype(np.float64))
        sine = np.sin(angle.astype(np.float64))
        out[0, :, at : at + quarter] = cosine
        out[0, :, at + quarter : at + 2 * quarter] = cosine
        out[1, :, at : at + quarter] = -sine
        out[2, :, at + quarter : at + 2 * quarter] = sine
        return out

    return half(grid_rows, 0), half(GRID_W, 2 * quarter)


def normed(values):
    mean = jnp.mean(values, axis=-1, keepdims=True)
    centered = values - mean
    variance = jnp.mean(centered * centered, axis=-1, keepdims=True)
    return centered * lax.rsqrt(variance + EPS)


def noise_level(index, count):
    frac = 1.0 - index / count
    lift = math.exp(TIME_SHIFT)
    return lift * frac / (lift * frac + 1.0 - frac)


def log_ratio(sigma):
    return jnp.log(1.0 - sigma) - jnp.log(sigma)


def kernel(
    sizes,
    img_hbm, txt_hbm, mod_hbm, wqkv_hbm, qg_hbm, kg_hbm, wout_hbm, bout_hbm, stale_hbm,
    fmod_hbm, wfin_hbm, bfin_hbm, lat_hbm, prev_hbm, rowtab_hbm, coltab_hbm,
    guidance, step_index, step_count,
    fresh_hbm, next_ref, den_ref,
    img, txt, mod, wqkv, qg, kg, bout, fmod, wfin, bfin, lat, prev, rowtab, coltab,
    modded, proj, tabs, fresh, qT, top, total, acc,
    fl, fr, wbuf, asend, arecv, mixed, final_in, vel, vel_in,
    in_sem, fresh_sem, ring_send, ring_recv, w_send, w_recv, d_send, d_recv, a_send, a_recv,
    v_send, v_recv,
):
    n_patch, n_head = sizes
    last = n_patch // 2
    p = lax.axis_index("patch")
    c = lax.axis_index("cfg")
    x = lax.axis_index("head")
    right, left = lax.rem(p + 1, n_patch), lax.rem(p + n_patch - 1, n_patch)
    other = 1 - c
    ups = [lax.rem(x + k, n_head) for k in range(n_head)]
    width = wout_hbm.shape[0]
    heads = width // HD
    depth = img.shape[1]
    rows = img.shape[0]
    trows = txt.shape[0]
    half_w = depth // 2
    out_rows = lat.shape[0]
    inv_root = HD ** (-0.5)

    pairs = [
        (img_hbm, img), (txt_hbm, txt), (mod_hbm, mod),
        (wqkv_hbm.at[0], wqkv.at[0]), (wqkv_hbm.at[1], wqkv.at[1]), (wqkv_hbm.at[2], wqkv.at[2]),
        (rowtab_hbm, rowtab), (coltab_hbm, coltab), (qg_hbm, qg), (kg_hbm, kg),
        (bout_hbm, bout), (fmod_hbm, fmod), (wfin_hbm, wfin), (bfin_hbm, bfin),
        (lat_hbm, lat), (prev_hbm, prev),
        (wout_hbm.at[:, pl.ds(0, half_w)], wbuf.at[0, pl.ds(0, width)]),
        (wout_hbm.at[:, pl.ds(half_w, half_w)], wbuf.at[1, pl.ds(0, width)]),
    ]
    reads = [pltpu.make_async_copy(s, d, in_sem.at[i]) for i, (s, d) in enumerate(pairs)]
    for r in reads:
        r.start()

    barrier = pltpu.get_barrier_semaphore()
    peers = [{"patch": right}, {"patch": left}, {"cfg": other}] + [{"head": u} for u in ups[1:]]
    for peer in peers:
        pl.semaphore_signal(barrier, inc=1, device_id=peer, device_id_type=MESH)
    pl.semaphore_wait(barrier, len(peers))

    def hop(side, stage, h, kv):
        if isinstance(stage, int) and stage == 1:
            src = stale_hbm.at[kv, :, pl.ds(pl.multiple_of(h * HD, HD), HD)]
        else:
            src = (fl, fr)[side].at[stage - 2, h, kv]
        if isinstance(stage, int) and stage == last:
            dst = fl.at[stage - 1, h, kv]
        else:
            dst = (fl, fr)[side].at[stage - 1, h, kv]
        return pltpu.make_async_remote_copy(
            src_ref=src, dst_ref=dst,
            send_sem=ring_send.at[side, stage - 1, h, kv],
            recv_sem=ring_recv.at[side, stage - 1, h, kv],
            device_id={"patch": (right, left)[side]}, device_id_type=MESH,
        )

    pieces = [(h, kv) for h in range(heads) for kv in range(2)]
    cut = len(pieces) // 2
    final_pieces = (pieces[:cut], pieces[cut:])

    for h, kv in pieces:
        for side in range(2):
            hop(side, 1, h, kv).start()

    def forward(stage, h):
        for kv in range(2):
            for side in range(2):
                hop(side, stage, h, kv).wait_recv()
                hop(side, stage + 1, h, kv).start()

    def w_copy(i, src, dst, send, recv, dev):
        return pltpu.make_async_remote_copy(
            src_ref=src, dst_ref=dst, send_sem=send.at[i], recv_sem=recv.at[i],
            device_id=dev, device_id_type=MESH,
        )

    my_cols = wout_hbm.at[:, pl.ds(pl.multiple_of(c * half_w, 128), half_w)]
    hw = width // 2
    w1 = w_copy(0, my_cols, wbuf.at[c, pl.ds(width, width)], w_send, w_recv, {"head": ups[1]})
    w3 = w_copy(1, my_cols, wbuf.at[c, pl.ds(3 * width, width)], w_send, w_recv, {"head": ups[3]})
    w2a = w_copy(2, wbuf.at[c, pl.ds(width, hw)], wbuf.at[c, pl.ds(2 * width, hw)],
                 w_send, w_recv, {"head": ups[1]})
    w2b = w_copy(3, wbuf.at[c, pl.ds(3 * width + hw, hw)], wbuf.at[c, pl.ds(2 * width + hw, hw)],
                 w_send, w_recv, {"head": ups[3]})
    d_out = [w_copy(k - 1, wbuf.at[c, pl.ds(k * width, width)], wbuf.at[c, pl.ds(k * width, width)],
                    d_send, d_recv, {"cfg": other}) for k in range(1, n_head)]
    d_in = [w_copy(k - 1, wbuf.at[other, pl.ds(k * width, width)],
                   wbuf.at[other, pl.ds(k * width, width)],
                   d_send, d_recv, {"cfg": other}) for k in range(1, n_head)]
    w1.start()
    w3.start()

    for r in reads[:3]:
        r.wait()
    block = 16

    def modulate(values):
        return (normed(values.astype(F32)) * (1.0 + mod[1]) + mod[0]).astype(BF)

    for i in range(trows // block):
        modded[pl.ds(i * block, block), :] = modulate(txt[pl.ds(i * block, block), :])

    def modulate_rows(i, carry):
        at = pl.multiple_of(i * block, block)
        modded[pl.ds(trows + at, block), :] = modulate(img[pl.ds(at, block), :])
        return carry

    lax.fori_loop(0, rows // block, modulate_rows, 0)

    def project(j, carry):
        pltpu.make_async_copy(wqkv_hbm.at[j], wqkv.at[j], in_sem.at[3 + j]).wait()
        proj[j] = jnp.dot(modded[...], wqkv[j], preferred_element_type=F32)
        return carry

    for j in range(3):
        project(j, 0)
        if j < heads:
            forward(1, j)
    for h in range(3, heads):
        forward(1, h)

    for r in reads[6:10]:
        r.wait()

    tabs[0, pl.ds(0, trows), :] = jnp.ones((trows, HD), F32)
    tabs[1, pl.ds(0, trows), :] = jnp.zeros((trows, HD), F32)
    tabs[2, pl.ds(0, trows), :] = jnp.zeros((trows, HD), F32)
    grid_rows = rows // GRID_W
    for t in range(3):
        for i in range(grid_rows):
            tabs[t, pl.ds(trows + i * GRID_W, GRID_W), :] = (
                coltab[t] + rowtab[t, pl.ds(p * grid_rows + i, 1), :]
            )

    quarter = HD // 4

    def turned(values, gain, first):
        scaled = values * lax.rsqrt(jnp.mean(values * values, axis=-1, keepdims=True) + EPS) * gain
        n = values.shape[0]
        return (
            scaled * tabs[0, pl.ds(first, n), :]
            + pltpu.roll(scaled, HD - quarter, 1) * tabs[1, pl.ds(first, n), :]
            + pltpu.roll(scaled, quarter, 1) * tabs[2, pl.ds(first, n), :]
        )

    for h in range(heads):
        cols = pl.ds(h * HD, HD)
        q = turned(proj[0, pl.ds(trows, rows), cols], qg[...], trows).astype(BF)
        qT[h] = q.T
        fresh[0, :, cols] = turned(proj[1, :, cols], kg[...], 0).astype(BF)
    fresh[1] = proj[2].astype(BF)
    fresh_out = pltpu.make_async_copy(fresh, fresh_hbm, fresh_sem.at[0])
    fresh_out.start()

    top[...] = jnp.full(top.shape, -1e30, F32)
    total[...] = jnp.zeros(total.shape, F32)
    acc[...] = jnp.zeros(acc.shape, F32)

    def attend(h, keys, vals):
        scores = jnp.dot(keys, qT[h], preferred_element_type=F32)
        old = top[h]
        new = jnp.maximum(old, jnp.max(scores, axis=0, keepdims=True))
        expo = jnp.exp((scores - new) * inv_root)
        factor = jnp.exp((old - new) * inv_root)
        top[h] = new
        total[h] = total[h] * factor + jnp.sum(expo, axis=0, keepdims=True)
        acc[h] = acc[h] * factor + lax.dot_general(
            vals, expo.astype(BF), (((0,), (0,)), ((), ())), preferred_element_type=F32
        )

    for h in range(heads):
        cols = pl.ds(h * HD, HD)
        attend(h, fresh[0, :, cols], fresh[1, :, cols])

    def both(stage, h):
        attend(h, fl[stage - 1, h, 0], fl[stage - 1, h, 1])
        attend(h, fr[stage - 1, h, 0], fr[stage - 1, h, 1])

    def step(stage, carry):
        def one(h, inner):
            forward(stage + 1, h)
            both(stage, h)
            return inner

        return lax.fori_loop(0, heads, one, carry)

    relay = (last - 2) // 2 + 1
    lax.fori_loop(1, relay, step, 0)
    w1.wait_recv()
    w2a.start()
    d_out[0].start()
    w3.wait_recv()
    w2b.start()
    d_out[2].start()
    lax.fori_loop(relay, last - 2, step, 0)

    for h in range(heads):
        for kv in range(2):
            for side in range(2):
                hop(side, last - 1, h, kv).wait_recv()
                if (h, kv) in final_pieces[side]:
                    hop(side, last, h, kv).start()
        both(last - 2, h)

    w2a.wait_recv()
    w2b.wait_recv()
    d_out[1].start()
    for r in reads[10:]:
        r.wait()

    def nearer(h, carry):
        both(last - 1, h)
        return carry

    lax.fori_loop(0, heads, nearer, 0)
    for copy in d_in:
        copy.wait_recv()

    for h in range(heads):
        for kv in range(2):
            for side in range(2):
                if (h, kv) in final_pieces[side]:
                    hop(side, last, h, kv).wait_recv()
        attend(h, fl[last - 1, h, 0], fl[last - 1, h, 1])
        out = (acc[h] / total[h]).astype(BF).T
        for part in range(2):
            for k in range(n_head):
                at = part * n_head * out_rows + k * out_rows
                asend[k, pl.ds(part * out_rows, out_rows), pl.ds(h * HD, HD)] = (
                    out[at : at + out_rows, :]
                )

    a_copies = [
        pltpu.make_async_remote_copy(
            src_ref=asend.at[ups[k]], dst_ref=arecv.at[:, pl.ds(k * width, width)],
            send_sem=a_send.at[k - 1], recv_sem=a_recv.at[k - 1],
            device_id={"head": ups[k]}, device_id_type=MESH,
        )
        for k in range(1, n_head)
    ]
    for k in (2, 1, 3):
        a_copies[k - 1].start()
    arecv[:, pl.ds(0, width)] = asend[x]
    for copy in a_copies:
        copy.wait_recv()

    chunk = 512
    attn = arecv[...]
    for n in range(depth // chunk):
        half, at = divmod(n * chunk, half_w)
        cols = pl.ds(n * chunk, chunk)
        projected = jnp.dot(attn, wbuf[half, :, pl.ds(at, chunk)], preferred_element_type=F32)
        for part in range(2):
            own = pl.ds(pl.multiple_of(part * n_head * out_rows + x * out_rows, out_rows), out_rows)
            mixed[pl.ds(part * out_rows, out_rows), cols] = img[own, cols].astype(F32) + mod[
                2, :, cols
            ] * (projected[part * out_rows : (part + 1) * out_rows] + bout[:, cols])

    def finish(i, carry):
        at = pl.multiple_of(i * block, block)
        final_in[pl.ds(at, block), :] = (
            normed(mixed[pl.ds(at, block), :]) * (1.0 + fmod[1:2, :]) + fmod[0:1, :]
        ).astype(BF)
        return carry

    lax.fori_loop(0, 2 * out_rows // block, finish, 0)
    velocity = (
        lax.dot_general(
            final_in[...], wfin[...], (((1,), (1,)), ((), ())), preferred_element_type=F32
        )
        + bfin[...]
    )
    ch = velocity.shape[1]
    vel[...] = jnp.zeros(vel.shape, F32)
    vel[0, :, pl.ds(0, ch)] = velocity[:out_rows]
    vel[1, :, pl.ds(0, ch)] = velocity[out_rows:]
    swap = pltpu.make_async_remote_copy(
        src_ref=vel.at[other], dst_ref=vel_in, send_sem=v_send.at[0], recv_sem=v_recv.at[0],
        device_id={"cfg": other}, device_id_type=MESH,
    )
    swap.start()

    index = jnp.full((1, ch), step_index[0], jnp.int32).astype(F32)
    count = jnp.full((1, ch), step_count[0], jnp.int32).astype(F32)
    scale = jnp.full((1, ch), guidance[0], F32)
    sigma_prev = noise_level(index - 1.0, count)
    sigma_now = noise_level(index, count)
    sigma_next = noise_level(index + 1.0, count)
    step_now = log_ratio(sigma_next) - log_ratio(sigma_now)
    step_prev = log_ratio(sigma_now) - log_ratio(sigma_prev)
    ratio = step_prev / step_now
    swap.wait_recv()
    mine = vel[c, :, pl.ds(0, ch)]
    theirs = vel_in[:, pl.ds(0, ch)]
    cond = jnp.where(c == 0, mine, theirs)
    uncond = jnp.where(c == 0, theirs, mine)
    guided = uncond + scale * (cond - uncond)
    denoised = lat[...] - sigma_now * guided
    blend = (1.0 + 0.5 / ratio) * denoised - 0.5 / ratio * prev[...]
    next_ref[...] = (
        sigma_next / sigma_now * lat[...] - (1.0 - sigma_next) * (jnp.exp(-step_now) - 1.0) * blend
    )
    den_ref[...] = denoised

    fresh_out.wait()
    for h, kv in pieces:
        for side in range(2):
            hop(side, 1, h, kv).wait_send()

    def drain(stage, carry):
        for h, kv in pieces:
            for side in range(2):
                hop(side, stage, h, kv).wait_send()
        return carry

    lax.fori_loop(2, last, drain, 0)
    for side in range(2):
        for h, kv in final_pieces[side]:
            hop(side, last, h, kv).wait_send()
    for copy in (w1, w3, w2a, w2b, *d_out, *a_copies, swap):
        copy.wait_send()


def body(
    sizes,
    img_hidden, txt_hidden, modulation, w_qkv, q_gain, k_gain, w_out, b_out, stale_kv,
    final_mod, w_final, b_final, latent, prev_denoised, guidance, step_index, step_count,
):
    n_patch, n_head = sizes
    rows, depth = img_hidden.shape[1:]
    trows = txt_hidden.shape[1]
    kv_rows = rows + trows
    width = w_out.shape[0]
    heads = width // HD
    out_rows, ch = latent.shape
    last = n_patch // 2
    n_rows = n_patch * rows // GRID_W
    rowtab, coltab = rotation_tables(n_rows)
    any_spec = pl.BlockSpec(memory_space=pl.ANY)
    smem = pl.BlockSpec(memory_space=pltpu.SMEM)
    vmem = pl.BlockSpec(memory_space=pltpu.VMEM)
    dma = pltpu.SemaphoreType.DMA
    V = pltpu.VMEM
    outs = pl.pallas_call(
        functools.partial(kernel, sizes),
        out_shape=(
            jax.ShapeDtypeStruct((2, kv_rows, width), BF),
            jax.ShapeDtypeStruct((out_rows, ch), F32),
            jax.ShapeDtypeStruct((out_rows, ch), F32),
        ),
        in_specs=[any_spec] * 16 + [smem] * 3,
        out_specs=(any_spec, vmem, vmem),
        scratch_shapes=[
            V((rows, depth), BF), V((trows, depth), BF), V((3, 1, depth), F32),
            V((3, depth, width), BF), V((1, HD), F32), V((1, HD), F32), V((1, depth), F32),
            V((2, depth), F32), V((ch, depth), BF), V((1, ch), F32), V((out_rows, ch), F32),
            V((out_rows, ch), F32), V((3, n_rows, HD), F32), V((3, GRID_W, HD), F32),
            V((kv_rows, depth), BF), V((3, kv_rows, width), F32), V((3, kv_rows, HD), F32),
            V((2, kv_rows, width), BF), V((heads, HD, rows), BF), V((heads, 1, rows), F32),
            V((heads, 1, rows), F32), V((heads, HD, rows), F32),
            V((last, heads, 2, kv_rows, HD), BF), V((last - 1, heads, 2, kv_rows, HD), BF),
            V((2, n_head * width, depth // 2), BF),
            V((n_head, 2 * out_rows, width), BF), V((2 * out_rows, n_head * width), BF),
            V((2 * out_rows, depth), F32), V((2 * out_rows, depth), BF),
            V((2, out_rows, 128), F32), V((out_rows, 128), F32),
            dma((18,)), dma((1,)),
            dma((2, last, heads, 2)), dma((2, last, heads, 2)),
            dma((4,)), dma((4,)), dma((n_head - 1,)), dma((n_head - 1,)),
            dma((n_head - 1,)), dma((n_head - 1,)), dma((1,)), dma((1,)),
        ],
        compiler_params=pltpu.CompilerParams(
            collective_id=0, has_side_effects=True, vmem_limit_bytes=60 * 1024 * 1024
        ),
    )(
        img_hidden[0], txt_hidden[0], modulation.transpose(1, 0, 2), w_qkv.transpose(1, 0, 2),
        q_gain[None], k_gain[None], w_out, b_out[None], stale_kv[0], final_mod[0], w_final.T,
        b_final[None], latent, prev_denoised, jnp.asarray(rowtab), jnp.asarray(coltab),
        guidance, step_index, step_count,
    )
    return outs[0][None], outs[1], outs[2]


def solution(mesh):
    sizes = (mesh.shape["patch"], mesh.shape["head"])
    rows4 = P(("groups", "patch", "cfg", "head"), None)
    return jax.shard_map(
        functools.partial(body, sizes),
        mesh=mesh,
        in_specs=(
            P("cfg", ("groups", "patch"), None),
            P("cfg", ("groups", "patch"), None),
            P(("groups", "cfg"), None, None),
            P(None, None, "head"),
            P(),
            P(),
            P("head", None),
            P(),
            P("cfg", None, ("groups", "patch"), "head"),
            P(("groups", "cfg"), None, None),
            P(),
            P(),
            rows4,
            rows4,
            P("groups"),
            P(),
            P(),
        ),
        out_specs=(P("cfg", None, ("groups", "patch"), "head"), rows4, rows4),
        check_vma=False,
    )
```

```python
import functools
import math

import jax
import jax.numpy as jnp
import numpy as np
from jax import lax
from jax.experimental import pallas as pl
from jax.experimental.pallas import tpu as pltpu
from jax.sharding import PartitionSpec as P

HD = 128
GRID_W = 128
EPS = 1e-06
TIME_SHIFT = 3.0
MESH = pl.DeviceIdType.MESH
BF = jnp.bfloat16
F32 = jnp.float32


def rotation_tables(grid_rows):
    quarter = HD // 4
    freqs = 10000.0 ** (-np.arange(quarter, dtype=np.float32) / quarter)
    freqs = freqs.astype(np.float32)

    def half(count, at):
        angle = np.arange(count, dtype=np.float32)[:, None] * freqs[None, :]
        out = np.zeros((3, count, HD), np.float32)
        cosine = np.cos(angle.astype(np.float64))
        sine = np.sin(angle.astype(np.float64))
        out[0, :, at : at + quarter] = cosine
        out[0, :, at + quarter : at + 2 * quarter] = cosine
        out[1, :, at : at + quarter] = -sine
        out[2, :, at + quarter : at + 2 * quarter] = sine
        return out

    return half(grid_rows, 0), half(GRID_W, 2 * quarter)


def normed(values):
    mean = jnp.mean(values, axis=-1, keepdims=True)
    centered = values - mean
    variance = jnp.mean(centered * centered, axis=-1, keepdims=True)
    return centered * lax.rsqrt(variance + EPS)


def noise_level(index, count):
    frac = 1.0 - index / count
    lift = math.exp(TIME_SHIFT)
    return lift * frac / (lift * frac + 1.0 - frac)


def log_ratio(sigma):
    return jnp.log(1.0 - sigma) - jnp.log(sigma)


def kernel(
    sizes,
    img_hbm, txt_hbm, mod_hbm, wqkv_hbm, qg_hbm, kg_hbm, wout_hbm, bout_hbm, stale_hbm,
    fmod_hbm, wfin_hbm, bfin_hbm, lat_hbm, prev_hbm, rowtab_hbm, coltab_hbm,
    plan_hbm,
    fresh_hbm, next_ref, den_ref,
    own, img, txt, mod, wqkv, qg, kg, bout, fmod, wfin, bfin, lat, prev, rowtab, coltab,
    plan, modded, proj, tabs, fresh, qT, top, total, acc,
    fl, fr, wbuf, asend, arecv, partial, mixed, final_in, vel, vel_in,
    own_sem, in_sem, fresh_sem, ring_send, ring_recv, w_send, w_recv, d_send, d_recv, a_send, a_recv,
    v_send, v_recv,
):
    n_patch, n_head = sizes
    last = n_patch // 2
    p = lax.axis_index("patch")
    c = lax.axis_index("cfg")
    x = lax.axis_index("head")
    right, left = lax.rem(p + 1, n_patch), lax.rem(p + n_patch - 1, n_patch)
    other = 1 - c
    ups = [lax.rem(x + k, n_head) for k in range(n_head)]
    heads = wout_hbm.shape[0]
    depth = img.shape[1]
    rows = img.shape[0]
    trows = txt.shape[0]
    half_w = depth // 2
    out_rows = lat.shape[0]
    inv_root = HD ** (-0.5)

    mine = [
        pltpu.make_async_copy(
            stale_hbm.at[kv, :, pl.ds(h * HD, HD)], own.at[h, kv], own_sem.at[h, kv]
        )
        for h in range(heads)
        for kv in range(2)
    ]
    for copy in mine:
        copy.start()
    pairs = [
        (img_hbm, img), (txt_hbm, txt), (mod_hbm, mod),
        (wqkv_hbm.at[0], wqkv.at[0]), (wqkv_hbm.at[1], wqkv.at[1]), (wqkv_hbm.at[2], wqkv.at[2]),
        (rowtab_hbm, rowtab), (coltab_hbm, coltab), (qg_hbm, qg), (kg_hbm, kg),
        (bout_hbm, bout), (fmod_hbm, fmod), (wfin_hbm, wfin), (bfin_hbm, bfin),
        (lat_hbm, lat), (prev_hbm, prev),
        (plan_hbm, plan),
        (wout_hbm.at[:, :, pl.ds(0, half_w)], wbuf.at[0, :, 0]),
        (wout_hbm.at[:, :, pl.ds(half_w, half_w)], wbuf.at[1, :, 0]),
    ]
    reads = [pltpu.make_async_copy(s, d, in_sem.at[i]) for i, (s, d) in enumerate(pairs)]
    for r in reads:
        r.start()

    barrier = pltpu.get_barrier_semaphore()
    peers = [{"patch": right}, {"patch": left}, {"cfg": other}] + [{"head": u} for u in ups[1:]]
    for peer in peers:
        pl.semaphore_signal(barrier, inc=1, device_id=peer, device_id_type=MESH)
    pl.semaphore_wait(barrier, len(peers))

    def hop(side, stage, h, kv=None):
        at = (h,) if kv is None else (h, kv)
        first = isinstance(stage, int) and stage == 1
        end = isinstance(stage, int) and stage == last
        src = own.at[at] if first else (fl, fr)[side].at[(stage - 2, *at)]
        dst = (fl if end else (fl, fr)[side]).at[(stage - 1, *at)]
        return pltpu.make_async_remote_copy(
            src_ref=src, dst_ref=dst,
            send_sem=ring_send.at[side, stage - 1, h],
            recv_sem=ring_recv.at[side, stage - 1, h],
            device_id={"patch": (right, left)[side]}, device_id_type=MESH,
        )

    middle = heads // 2
    final_pieces = (
        [(h, None) for h in range(middle)] + [(middle, 0)],
        [(h, None) for h in range(middle + 1, heads)] + [(middle, 1)],
    )

    for h in range(heads):
        mine[2 * h].wait()
        mine[2 * h + 1].wait()
        for side in range(2):
            hop(side, 1, h).start()

    def forward(stage, h):
        for side in range(2):
            hop(side, stage, h).wait_recv()
            hop(side, stage + 1, h).start()

    def w_copy(i, src, dst, send, recv, dev):
        return pltpu.make_async_remote_copy(
            src_ref=src, dst_ref=dst, send_sem=send.at[i], recv_sem=recv.at[i],
            device_id=dev, device_id_type=MESH,
        )

    my_cols = wout_hbm.at[:, :, pl.ds(pl.multiple_of(c * half_w, 128), half_w)]
    hd2 = HD // 2
    w1 = w_copy(0, my_cols, wbuf.at[c, :, 1], w_send, w_recv, {"head": ups[1]})
    w3 = w_copy(1, my_cols, wbuf.at[c, :, 3], w_send, w_recv, {"head": ups[3]})
    w2a = w_copy(2, wbuf.at[c, :, 1, pl.ds(0, hd2)], wbuf.at[c, :, 2, pl.ds(0, hd2)],
                 w_send, w_recv, {"head": ups[1]})
    w2b = w_copy(3, wbuf.at[c, :, 3, pl.ds(hd2, hd2)], wbuf.at[c, :, 2, pl.ds(hd2, hd2)],
                 w_send, w_recv, {"head": ups[3]})
    d_out = [w_copy(k - 1, wbuf.at[c, :, k], wbuf.at[c, :, k], d_send, d_recv, {"cfg": other})
             for k in range(1, n_head)]
    d_in = [w_copy(k - 1, wbuf.at[other, :, k], wbuf.at[other, :, k], d_send, d_recv,
                   {"cfg": other}) for k in range(1, n_head)]
    w1.start()
    w3.start()

    for r in reads[:3]:
        r.wait()
    block = 16

    def modulate(values):
        return (normed(values.astype(F32)) * (1.0 + mod[1]) + mod[0]).astype(BF)

    for i in range(trows // block):
        modded[pl.ds(i * block, block), :] = modulate(txt[pl.ds(i * block, block), :])

    def modulate_rows(i, carry):
        at = pl.multiple_of(i * block, block)
        modded[pl.ds(trows + at, block), :] = modulate(img[pl.ds(at, block), :])
        return carry

    lax.fori_loop(0, rows // block, modulate_rows, 0)

    def project(j, carry):
        pltpu.make_async_copy(wqkv_hbm.at[j], wqkv.at[j], in_sem.at[3 + j]).wait()
        proj[j] = jnp.dot(modded[...], wqkv[j], preferred_element_type=F32)
        return carry

    for j in range(3):
        project(j, 0)
        if j < heads:
            forward(1, j)
    for h in range(3, heads):
        forward(1, h)

    for r in reads[6:10]:
        r.wait()

    tabs[0, pl.ds(0, trows), :] = jnp.ones((trows, HD), F32)
    tabs[1, pl.ds(0, trows), :] = jnp.zeros((trows, HD), F32)
    tabs[2, pl.ds(0, trows), :] = jnp.zeros((trows, HD), F32)
    grid_rows = rows // GRID_W
    for t in range(3):
        for i in range(grid_rows):
            tabs[t, pl.ds(trows + i * GRID_W, GRID_W), :] = (
                coltab[t] + rowtab[t, pl.ds(p * grid_rows + i, 1), :]
            )

    quarter = HD // 4

    def turned(values, gain, first):
        scaled = values * lax.rsqrt(jnp.mean(values * values, axis=-1, keepdims=True) + EPS) * gain
        n = values.shape[0]
        return (
            scaled * tabs[0, pl.ds(first, n), :]
            + pltpu.roll(scaled, HD - quarter, 1) * tabs[1, pl.ds(first, n), :]
            + pltpu.roll(scaled, quarter, 1) * tabs[2, pl.ds(first, n), :]
        )

    for h in range(heads):
        cols = pl.ds(h * HD, HD)
        q = turned(proj[0, pl.ds(trows, rows), cols], qg[...], trows).astype(BF)
        qT[h] = q.T
        fresh[0, :, cols] = turned(proj[1, :, cols], kg[...], 0).astype(BF)
    fresh[1] = proj[2].astype(BF)
    fresh_out = pltpu.make_async_copy(fresh, fresh_hbm, fresh_sem.at[0])
    fresh_out.start()

    top[...] = jnp.full(top.shape, -1e30, F32)
    total[...] = jnp.zeros(total.shape, F32)
    acc[...] = jnp.zeros(acc.shape, F32)

    def attend(h, keys, vals):
        scores = jnp.dot(keys, qT[h], preferred_element_type=F32)
        old = top[h]
        new = jnp.maximum(old, jnp.max(scores, axis=0, keepdims=True))
        expo = jnp.exp((scores - new) * inv_root)
        factor = jnp.exp((old - new) * inv_root)
        top[h] = new
        total[h] = total[h] * factor + jnp.sum(expo, axis=0, keepdims=True)
        acc[h] = acc[h] * factor + lax.dot_general(
            vals, expo.astype(BF), (((0,), (0,)), ((), ())), preferred_element_type=F32
        )

    for h in range(heads):
        cols = pl.ds(h * HD, HD)
        attend(h, fresh[0, :, cols], fresh[1, :, cols])

    def both(stage, h):
        attend(h, fl[stage - 1, h, 0], fl[stage - 1, h, 1])
        attend(h, fr[stage - 1, h, 0], fr[stage - 1, h, 1])

    def step(stage, carry):
        def one(h, inner):
            forward(stage + 1, h)
            both(stage, h)
            return inner

        return lax.fori_loop(0, heads, one, carry)

    relay = (last - 2) // 2 + 1
    lax.fori_loop(1, relay, step, 0)
    w1.wait_recv()
    w2a.start()
    d_out[0].start()
    w3.wait_recv()
    w2b.start()
    d_out[2].start()
    lax.fori_loop(relay, last - 2, step, 0)

    for h in range(heads):
        for side in range(2):
            hop(side, last - 1, h).wait_recv()
        both(last - 2, h)
    for side in range(2):
        for h, kv in final_pieces[side]:
            hop(side, last, h, kv).start()

    w2a.wait_recv()
    w2b.wait_recv()
    d_out[1].start()
    for r in reads[10:]:
        r.wait()

    def nearer(h, carry):
        both(last - 1, h)
        return carry

    lax.fori_loop(0, heads, nearer, 0)
    for copy in d_in:
        copy.wait_recv()

    def a_copy(h, k):
        return pltpu.make_async_remote_copy(
            src_ref=asend.at[h, ups[k]], dst_ref=arecv.at[h, :, pl.ds(k * HD, HD)],
            send_sem=a_send.at[h, k - 1], recv_sem=a_recv.at[h, k - 1],
            device_id={"head": ups[k]}, device_id_type=MESH,
        )

    def end_of(h):
        for side in range(2):
            for at in final_pieces[side]:
                if at[0] == h:
                    hop(side, last, *at).wait_recv()
        attend(h, fl[last - 1, h, 0], fl[last - 1, h, 1])
        out = (acc[h] / total[h]).astype(BF).T
        for part in range(2):
            for k in range(n_head):
                at = part * n_head * out_rows + k * out_rows
                asend[h, k, pl.ds(part * out_rows, out_rows), :] = out[at : at + out_rows, :]
        for k in (2, 1, 3):
            a_copy(h, k).start()
        arecv[h, :, pl.ds(0, HD)] = asend[h, x]

    early = [h for h in range(heads) if h != middle]
    for h in early:
        end_of(h)
    end_of(middle)

    chunk = 512
    for h in early:
        for k in range(1, n_head):
            a_copy(h, k).wait_recv()
    for n in range(depth // chunk):
        half, at = divmod(n * chunk, half_w)
        cols = pl.ds(n * chunk, chunk)
        sums = bout[:, cols]
        for h in early:
            w = wbuf[half, h, :, :, pl.ds(at, chunk)].reshape(n_head * HD, chunk)
            sums = sums + jnp.dot(arecv[h], w, preferred_element_type=F32)
        partial[:, cols] = sums
    for k in range(1, n_head):
        a_copy(middle, k).wait_recv()
    for n in range(depth // chunk):
        half, at = divmod(n * chunk, half_w)
        cols = pl.ds(n * chunk, chunk)
        w = wbuf[half, middle, :, :, pl.ds(at, chunk)].reshape(n_head * HD, chunk)
        projected = partial[:, cols] + jnp.dot(arecv[middle], w, preferred_element_type=F32)
        for part in range(2):
            rows_of = pl.ds(
                pl.multiple_of(part * n_head * out_rows + x * out_rows, out_rows), out_rows
            )
            mixed[pl.ds(part * out_rows, out_rows), cols] = img[rows_of, cols].astype(F32) + mod[
                2, :, cols
            ] * projected[part * out_rows : (part + 1) * out_rows]

    def finish(i, carry):
        at = pl.multiple_of(i * block, block)
        final_in[pl.ds(at, block), :] = (
            normed(mixed[pl.ds(at, block), :]) * (1.0 + fmod[1:2, :]) + fmod[0:1, :]
        ).astype(BF)
        return carry

    lax.fori_loop(0, 2 * out_rows // block, finish, 0)
    velocity = (
        lax.dot_general(
            final_in[...], wfin[...], (((1,), (1,)), ((), ())), preferred_element_type=F32
        )
        + bfin[...]
    )
    ch = velocity.shape[1]
    vel[...] = jnp.zeros(vel.shape, F32)
    vel[0, :, pl.ds(0, ch)] = velocity[:out_rows]
    vel[1, :, pl.ds(0, ch)] = velocity[out_rows:]
    swap = pltpu.make_async_remote_copy(
        src_ref=vel.at[other], dst_ref=vel_in, send_sem=v_send.at[0], recv_sem=v_recv.at[0],
        device_id={"cfg": other}, device_id_type=MESH,
    )
    swap.start()

    index, count, scale = (plan[i : i + 1, pl.ds(0, ch)] for i in range(3))
    sigma_prev = noise_level(index - 1.0, count)
    sigma_now = noise_level(index, count)
    sigma_next = noise_level(index + 1.0, count)
    step_now = log_ratio(sigma_next) - log_ratio(sigma_now)
    step_prev = log_ratio(sigma_now) - log_ratio(sigma_prev)
    ratio = step_prev / step_now
    swap.wait_recv()
    ours = vel[c, :, pl.ds(0, ch)]
    theirs = vel_in[:, pl.ds(0, ch)]
    cond = jnp.where(c == 0, ours, theirs)
    uncond = jnp.where(c == 0, theirs, ours)
    guided = uncond + scale * (cond - uncond)
    denoised = lat[...] - sigma_now * guided
    blend = (1.0 + 0.5 / ratio) * denoised - 0.5 / ratio * prev[...]
    next_ref[...] = (
        sigma_next / sigma_now * lat[...] - (1.0 - sigma_next) * (jnp.exp(-step_now) - 1.0) * blend
    )
    den_ref[...] = denoised

    fresh_out.wait()
    for h in range(heads):
        for side in range(2):
            hop(side, 1, h).wait_send()

    def drain(stage, carry):
        for h in range(heads):
            for side in range(2):
                hop(side, stage, h).wait_send()
        return carry

    lax.fori_loop(2, last, drain, 0)
    for side in range(2):
        for h, kv in final_pieces[side]:
            hop(side, last, h, kv).wait_send()
    for h in range(heads):
        for k in range(1, n_head):
            a_copy(h, k).wait_send()
    for copy in (w1, w3, w2a, w2b, *d_out, swap):
        copy.wait_send()


def hand_over(*refs):
    n = 3
    ins, outs, held, sems = refs[:n], refs[n : 2 * n], refs[2 * n : 3 * n], refs[3 * n :]
    reads = [pltpu.make_async_copy(a, b, sems[0].at[i]) for i, (a, b) in enumerate(zip(ins, held))]
    writes = [pltpu.make_async_copy(a, b, sems[1].at[i]) for i, (a, b) in enumerate(zip(held, outs))]
    for copy in reads:
        copy.start()
    for i in range(n):
        reads[i].wait()
        writes[i].start()
    for copy in writes:
        copy.wait()


def body(
    sizes,
    img_hidden, txt_hidden, modulation, w_qkv, q_gain, k_gain, w_out, b_out, stale_kv,
    final_mod, w_final, b_final, latent, prev_denoised, guidance, step_index, step_count,
):
    n_patch, n_head = sizes
    rows, depth = img_hidden.shape[1:]
    trows = txt_hidden.shape[1]
    kv_rows = rows + trows
    width = w_out.shape[0]
    heads = width // HD
    out_rows, ch = latent.shape
    last = n_patch // 2
    n_rows = n_patch * rows // GRID_W
    rowtab, coltab = rotation_tables(n_rows)
    row = lax.broadcasted_iota(jnp.int32, (8, 128), 0)
    plan = jnp.where(
        row == 0, step_index.astype(F32), jnp.where(row == 1, step_count.astype(F32), guidance)
    )
    any_spec = pl.BlockSpec(memory_space=pl.ANY)
    vmem = pl.BlockSpec(memory_space=pltpu.VMEM)
    dma = pltpu.SemaphoreType.DMA
    V = pltpu.VMEM
    outs = pl.pallas_call(
        functools.partial(kernel, sizes),
        out_shape=(
            jax.ShapeDtypeStruct((2, kv_rows, width), BF),
            jax.ShapeDtypeStruct((out_rows, ch), F32),
            jax.ShapeDtypeStruct((out_rows, ch), F32),
        ),
        in_specs=[any_spec] * 17,
        out_specs=(any_spec, vmem, vmem),
        scratch_shapes=[
            V((heads, 2, kv_rows, HD), BF), V((rows, depth), BF), V((trows, depth), BF), V((3, 1, depth), F32),
            V((3, depth, width), BF), V((1, HD), F32), V((1, HD), F32), V((1, depth), F32),
            V((2, depth), F32), V((ch, depth), BF), V((1, ch), F32), V((out_rows, ch), F32),
            V((out_rows, ch), F32), V((3, n_rows, HD), F32), V((3, GRID_W, HD), F32),
            V((8, 128), F32),
            V((kv_rows, depth), BF), V((3, kv_rows, width), F32), V((3, kv_rows, HD), F32),
            V((2, kv_rows, width), BF), V((heads, HD, rows), BF), V((heads, 1, rows), F32),
            V((heads, 1, rows), F32), V((heads, HD, rows), F32),
            V((last, heads, 2, kv_rows, HD), BF), V((last - 1, heads, 2, kv_rows, HD), BF),
            V((2, heads, n_head, HD, depth // 2), BF),
            V((heads, n_head, 2 * out_rows, HD), BF), V((heads, 2 * out_rows, n_head * HD), BF),
            V((2 * out_rows, depth), F32), V((2 * out_rows, depth), F32),
            V((2 * out_rows, depth), BF),
            V((2, out_rows, 128), F32), V((out_rows, 128), F32),
            dma((heads, 2)), dma((19,)), dma((1,)),
            dma((2, last, heads)), dma((2, last, heads)),
            dma((4,)), dma((4,)), dma((n_head - 1,)), dma((n_head - 1,)),
            dma((heads, n_head - 1)), dma((heads, n_head - 1)), dma((1,)), dma((1,)),
        ],
        compiler_params=pltpu.CompilerParams(
            collective_id=0, has_side_effects=True, vmem_limit_bytes=60 * 1024 * 1024
        ),
    )(
        img_hidden[0], txt_hidden[0], modulation.transpose(1, 0, 2), w_qkv.transpose(1, 0, 2),
        q_gain[None], k_gain[None], w_out.reshape(heads, HD, depth), b_out[None], stale_kv[0], final_mod[0], w_final.T,
        b_final[None], latent, prev_denoised, jnp.asarray(rowtab), jnp.asarray(coltab),
        plan,
    )
    outs = pl.pallas_call(
        hand_over,
        out_shape=tuple(jax.ShapeDtypeStruct(o.shape, o.dtype) for o in outs),
        in_specs=[any_spec] * 3,
        out_specs=(any_spec,) * 3,
        scratch_shapes=[V(o.shape, o.dtype) for o in outs] + [dma((3,)), dma((3,))],
    )(*outs)
    return outs[0][None], outs[1], outs[2]


def solution(mesh):
    sizes = (mesh.shape["patch"], mesh.shape["head"])
    rows4 = P(("groups", "patch", "cfg", "head"), None)
    return jax.shard_map(
        functools.partial(body, sizes),
        mesh=mesh,
        in_specs=(
            P("cfg", ("groups", "patch"), None),
            P("cfg", ("groups", "patch"), None),
            P(("groups", "cfg"), None, None),
            P(None, None, "head"),
            P(),
            P(),
            P("head", None),
            P(),
            P("cfg", None, ("groups", "patch"), "head"),
            P(("groups", "cfg"), None, None),
            P(),
            P(),
            rows4,
            rows4,
            P("groups"),
            P(),
            P(),
        ),
        out_specs=(P("cfg", None, ("groups", "patch"), "head"), rows4, rows4),
        check_vma=False,
    )
```

```python
import functools
import math

import jax
import jax.numpy as jnp
import numpy as np
from jax import lax
from jax.experimental import pallas as pl
from jax.experimental.pallas import tpu as pltpu
from jax.sharding import PartitionSpec as P

HD = 128
GRID_W = 128
EPS = 1e-06
TIME_SHIFT = 3.0
MESH = pl.DeviceIdType.MESH
BF = jnp.bfloat16
F32 = jnp.float32


def rotation_tables(grid_rows):
    quarter = HD // 4
    freqs = 10000.0 ** (-np.arange(quarter, dtype=np.float32) / quarter)
    freqs = freqs.astype(np.float32)

    def half(count, at):
        angle = np.arange(count, dtype=np.float32)[:, None] * freqs[None, :]
        out = np.zeros((3, count, HD), np.float32)
        cosine = np.cos(angle.astype(np.float64))
        sine = np.sin(angle.astype(np.float64))
        out[0, :, at : at + quarter] = cosine
        out[0, :, at + quarter : at + 2 * quarter] = cosine
        out[1, :, at : at + quarter] = -sine
        out[2, :, at + quarter : at + 2 * quarter] = sine
        return out

    return half(grid_rows, 0), half(GRID_W, 2 * quarter)


def normed(values):
    mean = jnp.mean(values, axis=-1, keepdims=True)
    centered = values - mean
    variance = jnp.mean(centered * centered, axis=-1, keepdims=True)
    return centered * lax.rsqrt(variance + EPS)


def noise_level(index, count):
    frac = 1.0 - index / count
    lift = math.exp(TIME_SHIFT)
    return lift * frac / (lift * frac + 1.0 - frac)


def log_ratio(sigma):
    return jnp.log(1.0 - sigma) - jnp.log(sigma)


def kernel(
    sizes,
    img_hbm, txt_hbm, mod_hbm, wqkv_hbm, qg_hbm, kg_hbm, wout_hbm, bout_hbm, stale_hbm,
    fmod_hbm, wfin_hbm, bfin_hbm, lat_hbm, prev_hbm, rowtab_hbm, coltab_hbm,
    guidance_hbm, index_hbm, count_hbm,
    fresh_hbm, next_ref, den_ref,
    own, img, txt, mod, wqkv, qg, kg, bout, fmod, wfin, bfin, lat, prev, rowtab, coltab,
    guidance, step_index, step_count, modded, proj, tabs, fresh, qT, top, total, acc,
    fl, fr, wbuf, asend, arecv, partial, mixed, vel, vel_in,
    own_sem, in_sem, fresh_sem, ring_send, ring_recv, w_send, w_recv, d_send, d_recv, a_send, a_recv,
    v_send, v_recv,
):
    n_patch, n_head = sizes
    last = n_patch // 2
    p = lax.axis_index("patch")
    c = lax.axis_index("cfg")
    x = lax.axis_index("head")
    right, left = lax.rem(p + 1, n_patch), lax.rem(p + n_patch - 1, n_patch)
    other = 1 - c
    ups = [lax.rem(x + k, n_head) for k in range(n_head)]
    heads = wout_hbm.shape[0]
    assert heads == 3
    depth = img.shape[1]
    rows = img.shape[0]
    trows = txt.shape[0]
    half_w = depth // 2
    out_rows = lat.shape[0]
    inv_root = HD ** (-0.5)

    mine = [
        pltpu.make_async_copy(
            stale_hbm.at[kv, :, pl.ds(h * HD, HD)], own.at[h, kv], own_sem.at[h, kv]
        )
        for h in range(heads)
        for kv in range(2)
    ]
    for copy in mine:
        copy.start()
    pairs = [
        (img_hbm, img), (txt_hbm, txt), (mod_hbm, mod),
        (wqkv_hbm.at[0], wqkv.at[0]), (wqkv_hbm.at[1], wqkv.at[1]), (wqkv_hbm.at[2], wqkv.at[2]),
        (rowtab_hbm, rowtab), (coltab_hbm, coltab), (qg_hbm, qg), (kg_hbm, kg),
        (bout_hbm, bout), (fmod_hbm, fmod), (wfin_hbm, wfin), (bfin_hbm, bfin),
        (lat_hbm, lat), (prev_hbm, prev),
        (guidance_hbm, guidance), (index_hbm, step_index), (count_hbm, step_count),
        (wout_hbm.at[:, :, pl.ds(0, half_w)], wbuf.at[0, :, 0]),
        (wout_hbm.at[:, :, pl.ds(half_w, half_w)], wbuf.at[1, :, 0]),
    ]
    reads = [pltpu.make_async_copy(s, d, in_sem.at[i]) for i, (s, d) in enumerate(pairs)]
    for r in reads:
        r.start()

    barrier = pltpu.get_barrier_semaphore()
    peers = [{"patch": right}, {"patch": left}, {"cfg": other}] + [{"head": u} for u in ups[1:]]
    for peer in peers:
        pl.semaphore_signal(barrier, inc=1, device_id=peer, device_id_type=MESH)
    pl.semaphore_wait(barrier, len(peers))

    def hop(side, stage, h, kv=None):
        at = (h,) if kv is None else (h, kv)
        first = isinstance(stage, int) and stage == 1
        end = isinstance(stage, int) and stage == last
        src = own.at[at] if first else (fl, fr)[side].at[(stage - 2, *at)]
        dst = (fl if end else (fl, fr)[side]).at[(stage - 1, *at)]
        return pltpu.make_async_remote_copy(
            src_ref=src, dst_ref=dst,
            send_sem=ring_send.at[side, stage - 1, h],
            recv_sem=ring_recv.at[side, stage - 1, h],
            device_id={"patch": (right, left)[side]}, device_id_type=MESH,
        )

    middle = heads // 2
    final_pieces = (
        [(h, None) for h in range(middle)] + [(middle, 0)],
        [(h, None) for h in range(middle + 1, heads)] + [(middle, 1)],
    )

    def turn_of(side, i):
        return i if side == 0 else heads - 1 - i

    for copy in mine:
        copy.wait()
    for i in range(heads):
        for side in range(2):
            hop(side, 1, turn_of(side, i)).start()

    def forward(stage, i):
        for side in range(2):
            hop(side, stage, turn_of(side, i)).wait_recv()
            hop(side, stage + 1, turn_of(side, i)).start()

    def w_copy(i, src, dst, send, recv, dev):
        return pltpu.make_async_remote_copy(
            src_ref=src, dst_ref=dst, send_sem=send.at[i], recv_sem=recv.at[i],
            device_id=dev, device_id_type=MESH,
        )

    my_cols = wout_hbm.at[:, :, pl.ds(pl.multiple_of(c * half_w, 128), half_w)]
    hd2 = HD // 2
    w1 = w_copy(0, my_cols, wbuf.at[c, :, 1], w_send, w_recv, {"head": ups[1]})
    w3 = w_copy(1, my_cols, wbuf.at[c, :, 3], w_send, w_recv, {"head": ups[3]})
    w2a = w_copy(2, wbuf.at[c, :, 1, pl.ds(0, hd2)], wbuf.at[c, :, 2, pl.ds(0, hd2)],
                 w_send, w_recv, {"head": ups[1]})
    w2b = w_copy(3, wbuf.at[c, :, 3, pl.ds(hd2, hd2)], wbuf.at[c, :, 2, pl.ds(hd2, hd2)],
                 w_send, w_recv, {"head": ups[3]})
    d_out = [w_copy(k - 1, wbuf.at[c, :, k], wbuf.at[c, :, k], d_send, d_recv, {"cfg": other})
             for k in range(1, n_head)]
    d_in = [w_copy(k - 1, wbuf.at[other, :, k], wbuf.at[other, :, k], d_send, d_recv,
                   {"cfg": other}) for k in range(1, n_head)]
    w1.start()
    w3.start()

    for r in reads[:3]:
        r.wait()
    block = 16

    def modulate(values):
        return (normed(values.astype(F32)) * (1.0 + mod[1]) + mod[0]).astype(BF)

    for i in range(trows // block):
        modded[pl.ds(i * block, block), :] = modulate(txt[pl.ds(i * block, block), :])

    def modulate_rows(i, carry):
        at = pl.multiple_of(i * block, block)
        modded[pl.ds(trows + at, block), :] = modulate(img[pl.ds(at, block), :])
        return carry

    lax.fori_loop(0, rows // block, modulate_rows, 0)

    def project(j, carry):
        pltpu.make_async_copy(wqkv_hbm.at[j], wqkv.at[j], in_sem.at[3 + j]).wait()
        proj[j] = jnp.dot(modded[...], wqkv[j], preferred_element_type=F32)
        forward(1, j)
        return carry

    lax.fori_loop(0, heads, project, 0)
    for r in reads[6:10]:
        r.wait()

    tabs[0, pl.ds(0, trows), :] = jnp.ones((trows, HD), F32)
    tabs[1, pl.ds(0, trows), :] = jnp.zeros((trows, HD), F32)
    tabs[2, pl.ds(0, trows), :] = jnp.zeros((trows, HD), F32)
    grid_rows = rows // GRID_W
    for t in range(3):
        for i in range(grid_rows):
            tabs[t, pl.ds(trows + i * GRID_W, GRID_W), :] = (
                coltab[t] + rowtab[t, pl.ds(p * grid_rows + i, 1), :]
            )

    quarter = HD // 4

    def turned(values, gain, first):
        scaled = values * lax.rsqrt(jnp.mean(values * values, axis=-1, keepdims=True) + EPS) * gain
        n = values.shape[0]
        return (
            scaled * tabs[0, pl.ds(first, n), :]
            + pltpu.roll(scaled, HD - quarter, 1) * tabs[1, pl.ds(first, n), :]
            + pltpu.roll(scaled, quarter, 1) * tabs[2, pl.ds(first, n), :]
        )

    def turn(h, carry):
        cols = pl.ds(pl.multiple_of(h * HD, HD), HD)
        q = turned(proj[0, pl.ds(trows, rows), cols], qg[...], trows).astype(BF)
        qT[h] = q.T
        fresh[0, :, cols] = turned(proj[1, :, cols], kg[...], 0).astype(BF)
        return carry

    lax.fori_loop(0, heads, turn, 0)
    fresh[1] = proj[2].astype(BF)
    fresh_out = pltpu.make_async_copy(fresh, fresh_hbm, fresh_sem.at[0])
    fresh_out.start()

    top[...] = jnp.full(top.shape, -1e30, F32)
    total[...] = jnp.zeros(total.shape, F32)
    acc[...] = jnp.zeros(acc.shape, F32)

    def attend(h, keys, vals):
        scores = jnp.dot(keys, qT[h], preferred_element_type=F32)
        old = top[h]
        new = jnp.maximum(old, jnp.max(scores, axis=0, keepdims=True))
        expo = jnp.exp((scores - new) * inv_root)
        factor = jnp.exp((old - new) * inv_root)
        top[h] = new
        total[h] = total[h] * factor + jnp.sum(expo, axis=0, keepdims=True)
        acc[h] = acc[h] * factor + lax.dot_general(
            vals, expo.astype(BF), (((0,), (0,)), ((), ())), preferred_element_type=F32
        )

    def nearest(h, carry):
        cols = pl.ds(pl.multiple_of(h * HD, HD), HD)
        attend(h, fresh[0, :, cols], fresh[1, :, cols])
        return carry

    lax.fori_loop(0, heads, nearest, 0)

    def both(stage, i):
        for side, buffer in enumerate((fl, fr)):
            h = turn_of(side, i)
            attend(h, buffer[stage - 1, h, 0], buffer[stage - 1, h, 1])

    relay = (last - 2) // 2

    def step(i, carry):
        stage, j = i // heads + 1, lax.rem(i, heads)
        for side in range(2):
            hop(side, stage + 1, turn_of(side, j)).wait_recv()

        @pl.when(stage < last - 2)
        def _():
            for side in range(2):
                hop(side, stage + 2, turn_of(side, j)).start()

        @pl.when(jnp.logical_and(stage == last - 2, j < middle))
        def _():
            for side in range(2):
                hop(side, last, turn_of(side, j)).start()

        @pl.when(jnp.logical_and(stage == last - 2, j == middle))
        def _():
            for side in range(2):
                hop(side, last, middle, side).start()

        @pl.when(i == (relay - 1) * heads)
        def _():
            w1.wait_recv()
            w2a.start()
            d_out[0].start()
            w3.wait_recv()
            w2b.start()
            d_out[2].start()

        both(stage, j)
        return carry

    lax.fori_loop(0, (last - 2) * heads, step, 0)
    w2a.wait_recv()
    w2b.wait_recv()
    d_out[1].start()
    for r in reads[10:]:
        r.wait()

    def nearer(h, carry):
        both(last - 1, h)
        return carry

    lax.fori_loop(0, heads, nearer, 0)
    for copy in d_in:
        copy.wait_recv()

    def a_copy(h, k):
        return pltpu.make_async_remote_copy(
            src_ref=asend.at[h, ups[k]], dst_ref=arecv.at[h, :, pl.ds(k * HD, HD)],
            send_sem=a_send.at[h, k - 1], recv_sem=a_recv.at[h, k - 1],
            device_id={"head": ups[k]}, device_id_type=MESH,
        )

    def end_of(i, carry):
        h = lax.rem(2 * i, heads)
        for j in range(heads):

            @pl.when(i == j)
            def _(j=j):
                for side in range(2):
                    for at in final_pieces[side]:
                        if at[0] == 2 * j % heads:
                            hop(side, last, *at).wait_recv()

        attend(h, fl[last - 1, h, 0], fl[last - 1, h, 1])
        out = (acc[h] / total[h]).astype(BF).T
        for part in range(2):
            for k in range(n_head):
                at = part * n_head * out_rows + k * out_rows
                asend[h, k, pl.ds(part * out_rows, out_rows), :] = out[at : at + out_rows, :]
        for k in (2, 1, 3):
            a_copy(h, k).start()
        arecv[h, :, pl.ds(0, HD)] = asend[h, x]
        return carry

    lax.fori_loop(0, heads, end_of, 0)

    chunk = 512
    early = [h for h in range(heads) if h != middle]
    for h in early:
        for k in range(1, n_head):
            a_copy(h, k).wait_recv()

    def chunk_of(n):
        per_half = half_w // chunk
        at = pl.multiple_of(lax.rem(n, per_half) * chunk, chunk)
        return n // per_half, pl.ds(at, chunk), pl.ds(pl.multiple_of(n * chunk, chunk), chunk)

    def product(h, half, at):
        w = wbuf[half, h, :, :, at].reshape(n_head * HD, chunk)
        return jnp.dot(arecv[h], w, preferred_element_type=F32)

    def first_heads(n, carry):
        half, at, cols = chunk_of(n)
        sums = bout[:, cols]
        for h in early:
            sums = sums + product(h, half, at)
        partial[:, cols] = sums
        return carry

    lax.fori_loop(0, depth // chunk, first_heads, 0)
    for k in range(1, n_head):
        a_copy(middle, k).wait_recv()

    def last_head(n, carry):
        half, at, cols = chunk_of(n)
        projected = partial[:, cols] + product(middle, half, at)
        for part in range(2):
            rows_of = pl.ds(
                pl.multiple_of(part * n_head * out_rows + x * out_rows, out_rows), out_rows
            )
            mixed[pl.ds(part * out_rows, out_rows), cols] = img[rows_of, cols].astype(F32) + mod[
                2, :, cols
            ] * projected[part * out_rows : (part + 1) * out_rows]
        values = mixed[:, cols]
        for at in range(0, chunk, HD):
            carry = carry + values[:, at : at + HD]
        return carry

    sums = lax.fori_loop(0, depth // chunk, last_head, jnp.zeros((2 * out_rows, HD), F32))

    mean = jnp.sum(sums, axis=-1, keepdims=True) * (1.0 / depth)
    squares = jnp.zeros((2 * out_rows, HD), F32)
    for at in range(0, depth, HD):
        centered = mixed[:, pl.ds(at, HD)] - mean
        squares = squares + centered * centered
    scale = lax.rsqrt(jnp.sum(squares, axis=-1, keepdims=True) * (1.0 / depth) + EPS)
    velocity = bfin[...]
    for at in range(0, depth, chunk):
        cols = pl.ds(at, chunk)
        final_in = ((mixed[:, cols] - mean) * scale * (1.0 + fmod[1:2, cols]) + fmod[0:1, cols]).astype(BF)
        velocity = velocity + lax.dot_general(
            final_in, wfin[:, cols], (((1,), (1,)), ((), ())), preferred_element_type=F32
        )
    ch = velocity.shape[1]
    vel[...] = jnp.zeros(vel.shape, F32)
    vel[0, :, pl.ds(0, ch)] = velocity[:out_rows]
    vel[1, :, pl.ds(0, ch)] = velocity[out_rows:]
    swap = pltpu.make_async_remote_copy(
        src_ref=vel.at[other], dst_ref=vel_in, send_sem=v_send.at[0], recv_sem=v_recv.at[0],
        device_id={"cfg": other}, device_id_type=MESH,
    )
    swap.start()

    index = jnp.full((1, ch), step_index[0], jnp.int32).astype(F32)
    count = jnp.full((1, ch), step_count[0], jnp.int32).astype(F32)
    strength = jnp.full((1, ch), guidance[0], F32)
    sigma_prev = noise_level(index - 1.0, count)
    sigma_now = noise_level(index, count)
    sigma_next = noise_level(index + 1.0, count)
    step_now = log_ratio(sigma_next) - log_ratio(sigma_now)
    step_prev = log_ratio(sigma_now) - log_ratio(sigma_prev)
    ratio = step_prev / step_now
    swap.wait_recv()
    ours = vel[c, :, pl.ds(0, ch)]
    theirs = vel_in[:, pl.ds(0, ch)]
    cond = jnp.where(c == 0, ours, theirs)
    uncond = jnp.where(c == 0, theirs, ours)
    guided = uncond + strength * (cond - uncond)
    denoised = lat[...] - sigma_now * guided
    blend = (1.0 + 0.5 / ratio) * denoised - 0.5 / ratio * prev[...]
    next_ref[...] = (
        sigma_next / sigma_now * lat[...] - (1.0 - sigma_next) * (jnp.exp(-step_now) - 1.0) * blend
    )
    den_ref[...] = denoised

    fresh_out.wait()
    for h in range(heads):
        for side in range(2):
            hop(side, 1, h).wait_send()

    def drain(stage, carry):
        for h in range(heads):
            for side in range(2):
                hop(side, stage, h).wait_send()
        return carry

    lax.fori_loop(2, last, drain, 0)
    for side in range(2):
        for h, kv in final_pieces[side]:
            hop(side, last, h, kv).wait_send()
    for h in range(heads):
        for k in range(1, n_head):
            a_copy(h, k).wait_send()
    for copy in (w1, w3, w2a, w2b, *d_out, swap):
        copy.wait_send()


def hand_over(*refs):
    n = 3
    ins, outs, held, sems = refs[:n], refs[n : 2 * n], refs[2 * n : 3 * n], refs[3 * n :]
    reads = [pltpu.make_async_copy(a, b, sems[0].at[i]) for i, (a, b) in enumerate(zip(ins, held))]
    writes = [pltpu.make_async_copy(a, b, sems[1].at[i]) for i, (a, b) in enumerate(zip(held, outs))]
    for copy in reads:
        copy.start()
    for i in range(n):
        reads[i].wait()
        writes[i].start()
    for copy in writes:
        copy.wait()


def body(
    sizes,
    img_hidden, txt_hidden, modulation, w_qkv, q_gain, k_gain, w_out, b_out, stale_kv,
    final_mod, w_final, b_final, latent, prev_denoised, guidance, step_index, step_count,
):
    n_patch, n_head = sizes
    rows, depth = img_hidden.shape[1:]
    trows = txt_hidden.shape[1]
    kv_rows = rows + trows
    width = w_out.shape[0]
    heads = width // HD
    out_rows, ch = latent.shape
    last = n_patch // 2
    n_rows = n_patch * rows // GRID_W
    rowtab, coltab = rotation_tables(n_rows)
    any_spec = pl.BlockSpec(memory_space=pl.ANY)
    vmem = pl.BlockSpec(memory_space=pltpu.VMEM)
    dma = pltpu.SemaphoreType.DMA
    V = pltpu.VMEM
    outs = pl.pallas_call(
        functools.partial(kernel, sizes),
        out_shape=(
            jax.ShapeDtypeStruct((2, kv_rows, width), BF),
            jax.ShapeDtypeStruct((out_rows, ch), F32),
            jax.ShapeDtypeStruct((out_rows, ch), F32),
        ),
        in_specs=[any_spec] * 16 + [pl.BlockSpec(memory_space=pltpu.HBM)] * 3,
        out_specs=(any_spec, vmem, vmem),
        scratch_shapes=[
            V((heads, 2, kv_rows, HD), BF), V((rows, depth), BF), V((trows, depth), BF), V((3, 1, depth), F32),
            V((3, depth, width), BF), V((1, HD), F32), V((1, HD), F32), V((1, depth), F32),
            V((2, depth), F32), V((ch, depth), BF), V((1, ch), F32), V((out_rows, ch), F32),
            V((out_rows, ch), F32), V((3, n_rows, HD), F32), V((3, GRID_W, HD), F32),
            pltpu.SMEM((1,), F32), pltpu.SMEM((1,), jnp.int32), pltpu.SMEM((1,), jnp.int32),
            V((kv_rows, depth), BF), V((3, kv_rows, width), F32), V((3, kv_rows, HD), F32),
            V((2, kv_rows, width), BF), V((heads, HD, rows), BF), V((heads, 1, rows), F32),
            V((heads, 1, rows), F32), V((heads, HD, rows), F32),
            V((last, heads, 2, kv_rows, HD), BF), V((last - 1, heads, 2, kv_rows, HD), BF),
            V((2, heads, n_head, HD, depth // 2), BF),
            V((heads, n_head, 2 * out_rows, HD), BF), V((heads, 2 * out_rows, n_head * HD), BF),
            V((2 * out_rows, depth), F32), V((2 * out_rows, depth), F32),
            V((2, out_rows, 128), F32), V((out_rows, 128), F32),
            dma((heads, 2)), dma((21,)), dma((1,)),
            dma((2, last, heads)), dma((2, last, heads)),
            dma((4,)), dma((4,)), dma((n_head - 1,)), dma((n_head - 1,)),
            dma((heads, n_head - 1)), dma((heads, n_head - 1)), dma((1,)), dma((1,)),
        ],
        compiler_params=pltpu.CompilerParams(
            collective_id=0, has_side_effects=True, vmem_limit_bytes=60 * 1024 * 1024
        ),
    )(
        img_hidden[0], txt_hidden[0], modulation.transpose(1, 0, 2), w_qkv.transpose(1, 0, 2),
        q_gain[None], k_gain[None], w_out.reshape(heads, HD, depth), b_out[None], stale_kv[0], final_mod[0], w_final.T,
        b_final[None], latent, prev_denoised, jnp.asarray(rowtab), jnp.asarray(coltab),
        guidance, step_index, step_count,
    )
    outs = pl.pallas_call(
        hand_over,
        out_shape=tuple(jax.ShapeDtypeStruct(o.shape, o.dtype) for o in outs),
        in_specs=[any_spec] * 3,
        out_specs=(any_spec,) * 3,
        scratch_shapes=[V(o.shape, o.dtype) for o in outs] + [dma((3,)), dma((3,))],
    )(*outs)
    return outs[0][None], outs[1], outs[2]


def solution(mesh):
    sizes = (mesh.shape["patch"], mesh.shape["head"])
    rows4 = P(("groups", "patch", "cfg", "head"), None)
    return jax.shard_map(
        functools.partial(body, sizes),
        mesh=mesh,
        in_specs=(
            P("cfg", ("groups", "patch"), None),
            P("cfg", ("groups", "patch"), None),
            P(("groups", "cfg"), None, None),
            P(None, None, "head"),
            P(),
            P(),
            P("head", None),
            P(),
            P("cfg", None, ("groups", "patch"), "head"),
            P(("groups", "cfg"), None, None),
            P(),
            P(),
            rows4,
            rows4,
            P("groups"),
            P(),
            P(),
        ),
        out_specs=(P("cfg", None, ("groups", "patch"), "head"), rows4, rows4),
        check_vma=False,
    )
```

```python
import functools
import math

import jax
import jax.numpy as jnp
import numpy as np
from jax import lax
from jax.experimental import pallas as pl
from jax.experimental.pallas import tpu as pltpu
from jax.sharding import PartitionSpec as P

HD = 128
GRID_W = 128
EPS = 1e-06
TIME_SHIFT = 3.0
MESH = pl.DeviceIdType.MESH
BF = jnp.bfloat16
F32 = jnp.float32


def rotation_tables(grid_rows):
    quarter = HD // 4
    freqs = 10000.0 ** (-np.arange(quarter, dtype=np.float32) / quarter)
    freqs = freqs.astype(np.float32)

    def half(count, at):
        angle = np.arange(count, dtype=np.float32)[:, None] * freqs[None, :]
        out = np.zeros((3, count, HD), np.float32)
        cosine = np.cos(angle.astype(np.float64))
        sine = np.sin(angle.astype(np.float64))
        out[0, :, at : at + quarter] = cosine
        out[0, :, at + quarter : at + 2 * quarter] = cosine
        out[1, :, at : at + quarter] = -sine
        out[2, :, at + quarter : at + 2 * quarter] = sine
        return out

    return half(grid_rows, 0), half(GRID_W, 2 * quarter)


def normed(values):
    mean = jnp.mean(values, axis=-1, keepdims=True)
    centered = values - mean
    variance = jnp.mean(centered * centered, axis=-1, keepdims=True)
    return centered * lax.rsqrt(variance + EPS)


def noise_level(index, count):
    frac = 1.0 - index / count
    lift = math.exp(TIME_SHIFT)
    return lift * frac / (lift * frac + 1.0 - frac)


def log_ratio(sigma):
    return jnp.log(1.0 - sigma) - jnp.log(sigma)


def kernel(
    sizes,
    img_hbm, txt_hbm, mod_hbm, wqkv_hbm, qg_hbm, kg_hbm, wout_hbm, bout_hbm, stale_hbm,
    fmod_hbm, wfin_hbm, bfin_hbm, lat_hbm, prev_hbm, rowtab_hbm, coltab_hbm,
    guidance_hbm, index_hbm, count_hbm,
    fresh_hbm, next_ref, den_ref,
    own, img, txt, mod, wqkv, qg, kg, bout, fmod, wfin, bfin, lat, prev, rowtab, coltab,
    guidance, step_index, step_count, modded, proj, tabs, fresh, qT, top, total, acc,
    fl, fr, wbuf, asend, arecv, partial, mixed, hid_in, gate_in, fmod_in,
    own_sem, in_sem, fresh_sem, ring_send, ring_recv, w_send, w_recv, d_send, d_recv, a_send, a_recv,
    b_send, b_recv,
):
    n_patch, n_head = sizes
    last = n_patch // 2
    p = lax.axis_index("patch")
    c = lax.axis_index("cfg")
    x = lax.axis_index("head")
    right, left = lax.rem(p + 1, n_patch), lax.rem(p + n_patch - 1, n_patch)
    other = 1 - c
    ups = [lax.rem(x + k, n_head) for k in range(n_head)]
    heads = wout_hbm.shape[0]
    assert heads == 3
    depth = img.shape[1]
    rows = img.shape[0]
    trows = txt.shape[0]
    half_w = depth // 2
    out_rows = lat.shape[0]
    inv_root = HD ** (-0.5)

    mine = [
        pltpu.make_async_copy(
            stale_hbm.at[kv, :, pl.ds(h * HD, HD)], own.at[h, kv], own_sem.at[h, kv]
        )
        for h in range(heads)
        for kv in range(2)
    ]
    for copy in mine:
        copy.start()
    pairs = [
        (img_hbm, img), (txt_hbm, txt), (mod_hbm, mod),
        (wqkv_hbm.at[0], wqkv.at[0]), (wqkv_hbm.at[1], wqkv.at[1]), (wqkv_hbm.at[2], wqkv.at[2]),
        (rowtab_hbm, rowtab), (coltab_hbm, coltab), (qg_hbm, qg), (kg_hbm, kg),
        (bout_hbm, bout), (fmod_hbm, fmod), (wfin_hbm, wfin), (bfin_hbm, bfin),
        (lat_hbm, lat), (prev_hbm, prev),
        (guidance_hbm, guidance), (index_hbm, step_index), (count_hbm, step_count),
        (wout_hbm.at[:, :, pl.ds(0, half_w)], wbuf.at[0, :, 0]),
        (wout_hbm.at[:, :, pl.ds(half_w, half_w)], wbuf.at[1, :, 0]),
    ]
    reads = [pltpu.make_async_copy(s, d, in_sem.at[i]) for i, (s, d) in enumerate(pairs)]
    for r in reads:
        r.start()

    barrier = pltpu.get_barrier_semaphore()
    peers = [{"patch": right}, {"patch": left}, {"cfg": other}]
    peers += [{"head": u, "cfg": f} for u in ups[1:] for f in (c, other)]
    for peer in peers:
        pl.semaphore_signal(barrier, inc=1, device_id=peer, device_id_type=MESH)
    pl.semaphore_wait(barrier, len(peers))

    def hop(side, stage, h, kv=None):
        at = (h,) if kv is None else (h, kv)
        first = isinstance(stage, int) and stage == 1
        end = isinstance(stage, int) and stage == last
        src = own.at[at] if first else (fl, fr)[side].at[(stage - 2, *at)]
        dst = (fl if end else (fl, fr)[side]).at[(stage - 1, *at)]
        return pltpu.make_async_remote_copy(
            src_ref=src, dst_ref=dst,
            send_sem=ring_send.at[side, stage - 1, h],
            recv_sem=ring_recv.at[side, stage - 1, h],
            device_id={"patch": (right, left)[side]}, device_id_type=MESH,
        )

    middle = heads // 2
    final_pieces = (
        [(h, None) for h in range(middle)] + [(middle, 0)],
        [(h, None) for h in range(middle + 1, heads)] + [(middle, 1)],
    )

    def turn_of(side, i):
        return i if side == 0 else heads - 1 - i

    for copy in mine:
        copy.wait()
    for i in range(heads):
        for side in range(2):
            hop(side, 1, turn_of(side, i)).start()

    def forward(stage, i):
        for side in range(2):
            hop(side, stage, turn_of(side, i)).wait_recv()
            hop(side, stage + 1, turn_of(side, i)).start()

    def w_copy(i, src, dst, send, recv, dev):
        return pltpu.make_async_remote_copy(
            src_ref=src, dst_ref=dst, send_sem=send.at[i], recv_sem=recv.at[i],
            device_id=dev, device_id_type=MESH,
        )

    my_cols = wout_hbm.at[:, :, pl.ds(pl.multiple_of(c * half_w, 128), half_w)]
    hd2 = HD // 2
    w1 = w_copy(0, my_cols, wbuf.at[c, :, 1], w_send, w_recv, {"head": ups[1]})
    w3 = w_copy(1, my_cols, wbuf.at[c, :, 3], w_send, w_recv, {"head": ups[3]})
    w2a = w_copy(2, wbuf.at[c, :, 1, pl.ds(0, hd2)], wbuf.at[c, :, 2, pl.ds(0, hd2)],
                 w_send, w_recv, {"head": ups[1]})
    w2b = w_copy(3, wbuf.at[c, :, 3, pl.ds(hd2, hd2)], wbuf.at[c, :, 2, pl.ds(hd2, hd2)],
                 w_send, w_recv, {"head": ups[3]})
    d_out = [w_copy(k - 1, wbuf.at[c, :, k], wbuf.at[c, :, k], d_send, d_recv, {"cfg": other})
             for k in range(1, n_head)]
    d_in = [w_copy(k - 1, wbuf.at[other, :, k], wbuf.at[other, :, k], d_send, d_recv,
                   {"cfg": other}) for k in range(1, n_head)]
    w1.start()
    w3.start()

    def latent_rows(part):
        at = part * n_head * out_rows + x * out_rows
        return pl.ds(pl.multiple_of(at, out_rows), out_rows)

    b_copies = [
        w_copy(i, src, dst, b_send, b_recv, {"cfg": other})
        for i, (src, dst) in enumerate([
            (img_hbm.at[latent_rows(other)], hid_in), (mod_hbm.at[2], gate_in),
            (fmod_hbm, fmod_in),
        ])
    ]
    for copy in b_copies:
        copy.start()

    for r in reads[:3]:
        r.wait()
    block = 16

    def modulate(values):
        return (normed(values.astype(F32)) * (1.0 + mod[1]) + mod[0]).astype(BF)

    for i in range(trows // block):
        modded[pl.ds(i * block, block), :] = modulate(txt[pl.ds(i * block, block), :])

    def modulate_rows(i, carry):
        at = pl.multiple_of(i * block, block)
        modded[pl.ds(trows + at, block), :] = modulate(img[pl.ds(at, block), :])
        return carry

    lax.fori_loop(0, rows // block, modulate_rows, 0)

    def project(j, carry):
        pltpu.make_async_copy(wqkv_hbm.at[j], wqkv.at[j], in_sem.at[3 + j]).wait()
        proj[j] = jnp.dot(modded[...], wqkv[j], preferred_element_type=F32)
        forward(1, j)
        return carry

    lax.fori_loop(0, heads, project, 0)
    for r in reads[6:10]:
        r.wait()

    tabs[0, pl.ds(0, trows), :] = jnp.ones((trows, HD), F32)
    tabs[1, pl.ds(0, trows), :] = jnp.zeros((trows, HD), F32)
    tabs[2, pl.ds(0, trows), :] = jnp.zeros((trows, HD), F32)
    grid_rows = rows // GRID_W
    for t in range(3):
        for i in range(grid_rows):
            tabs[t, pl.ds(trows + i * GRID_W, GRID_W), :] = (
                coltab[t] + rowtab[t, pl.ds(p * grid_rows + i, 1), :]
            )

    quarter = HD // 4

    def turned(values, gain, first):
        scaled = values * lax.rsqrt(jnp.mean(values * values, axis=-1, keepdims=True) + EPS) * gain
        n = values.shape[0]
        return (
            scaled * tabs[0, pl.ds(first, n), :]
            + pltpu.roll(scaled, HD - quarter, 1) * tabs[1, pl.ds(first, n), :]
            + pltpu.roll(scaled, quarter, 1) * tabs[2, pl.ds(first, n), :]
        )

    def turn(h, carry):
        cols = pl.ds(pl.multiple_of(h * HD, HD), HD)
        q = turned(proj[0, pl.ds(trows, rows), cols], qg[...], trows).astype(BF)
        qT[h] = q.T
        fresh[0, :, cols] = turned(proj[1, :, cols], kg[...], 0).astype(BF)
        return carry

    lax.fori_loop(0, heads, turn, 0)
    fresh[1] = proj[2].astype(BF)
    fresh_out = pltpu.make_async_copy(fresh, fresh_hbm, fresh_sem.at[0])
    fresh_out.start()

    top[...] = jnp.full(top.shape, -1e30, F32)
    total[...] = jnp.zeros(total.shape, F32)
    acc[...] = jnp.zeros(acc.shape, F32)

    def attend(h, keys, vals):
        scores = jnp.dot(keys, qT[h], preferred_element_type=F32)
        old = top[h]
        new = jnp.maximum(old, jnp.max(scores, axis=0, keepdims=True))
        expo = jnp.exp((scores - new) * inv_root)
        factor = jnp.exp((old - new) * inv_root)
        top[h] = new
        total[h] = total[h] * factor + jnp.sum(expo, axis=0, keepdims=True)
        acc[h] = acc[h] * factor + lax.dot_general(
            vals, expo.astype(BF), (((0,), (0,)), ((), ())), preferred_element_type=F32
        )

    def nearest(h, carry):
        cols = pl.ds(pl.multiple_of(h * HD, HD), HD)
        attend(h, fresh[0, :, cols], fresh[1, :, cols])
        return carry

    lax.fori_loop(0, heads, nearest, 0)

    def both(stage, i):
        for side, buffer in enumerate((fl, fr)):
            h = turn_of(side, i)
            attend(h, buffer[stage - 1, h, 0], buffer[stage - 1, h, 1])

    relay = (last - 2) // 2

    def step(i, carry):
        stage, j = i // heads + 1, lax.rem(i, heads)
        for side in range(2):
            hop(side, stage + 1, turn_of(side, j)).wait_recv()

        @pl.when(stage < last - 2)
        def _():
            for side in range(2):
                hop(side, stage + 2, turn_of(side, j)).start()

        @pl.when(jnp.logical_and(stage == last - 2, j < middle))
        def _():
            for side in range(2):
                hop(side, last, turn_of(side, j)).start()

        @pl.when(jnp.logical_and(stage == last - 2, j == middle))
        def _():
            for side in range(2):
                hop(side, last, middle, side).start()

        @pl.when(i == (relay - 1) * heads)
        def _():
            w1.wait_recv()
            w2a.start()
            d_out[0].start()
            w3.wait_recv()
            w2b.start()
            d_out[2].start()

        both(stage, j)
        return carry

    lax.fori_loop(0, (last - 2) * heads, step, 0)
    w2a.wait_recv()
    w2b.wait_recv()
    d_out[1].start()
    for r in reads[10:]:
        r.wait()

    def nearer(h, carry):
        both(last - 1, h)
        return carry

    lax.fori_loop(0, heads, nearer, 0)
    for copy in d_in:
        copy.wait_recv()

    sides = (c, other)
    peers8 = [(f, k) for k in (2, 1, 3, 0) for f in range(2) if (f, k) != (0, 0)]

    def a_copy(h, f, k):
        dev = {"head": ups[k], "cfg": sides[f]}
        return pltpu.make_async_remote_copy(
            src_ref=asend.at[h, sides[f], ups[k]],
            dst_ref=arecv.at[h, f, :, pl.ds(k * HD, HD)],
            send_sem=a_send.at[h, f, k], recv_sem=a_recv.at[h, f, k],
            device_id=dev, device_id_type=MESH,
        )

    def end_of(i, carry):
        h = lax.rem(2 * i, heads)
        for j in range(heads):

            @pl.when(i == j)
            def _(j=j):
                for side in range(2):
                    for at in final_pieces[side]:
                        if at[0] == 2 * j % heads:
                            hop(side, last, *at).wait_recv()

        attend(h, fl[last - 1, h, 0], fl[last - 1, h, 1])
        out = (acc[h] / total[h]).astype(BF).T
        for part in range(2):
            for k in range(n_head):
                at = part * n_head * out_rows + k * out_rows
                asend[h, part, k] = out[at : at + out_rows, :]
        for f, k in peers8:
            a_copy(h, f, k).start()
        arecv[h, 0, :, pl.ds(0, HD)] = asend[h, c, x]
        return carry

    lax.fori_loop(0, heads, end_of, 0)

    chunk = 512
    early = [h for h in range(heads) if h != middle]
    for h in early:
        for f, k in peers8:
            a_copy(h, f, k).wait_recv()
    for copy in b_copies:
        copy.wait_recv()

    def chunk_of(n):
        per_half = half_w // chunk
        at = pl.multiple_of(lax.rem(n, per_half) * chunk, chunk)
        return n // per_half, pl.ds(at, chunk), pl.ds(pl.multiple_of(n * chunk, chunk), chunk)

    def product(h, half, at):
        w = wbuf[half, h, :, :, at].reshape(n_head * HD, chunk)
        return jnp.dot(
            arecv[h].reshape(2 * out_rows, n_head * HD), w, preferred_element_type=F32
        )

    def first_heads(n, carry):
        half, at, cols = chunk_of(n)
        sums = bout[:, cols]
        for h in early:
            sums = sums + product(h, half, at)
        partial[:, cols] = sums
        return carry

    lax.fori_loop(0, depth // chunk, first_heads, 0)
    for f, k in peers8:
        a_copy(middle, f, k).wait_recv()

    def last_head(n, carry):
        half, at, cols = chunk_of(n)
        projected = partial[:, cols] + product(middle, half, at)
        mixed[pl.ds(0, out_rows), cols] = (
            img[latent_rows(c), cols].astype(F32) + mod[2, :, cols] * projected[:out_rows]
        )
        mixed[pl.ds(out_rows, out_rows), cols] = (
            hid_in[:, cols].astype(F32) + gate_in[:, cols] * projected[out_rows:]
        )
        values = mixed[:, cols]
        for at in range(0, chunk, HD):
            carry = carry + values[:, at : at + HD]
        return carry

    sums = lax.fori_loop(0, depth // chunk, last_head, jnp.zeros((2 * out_rows, HD), F32))

    mean = jnp.sum(sums, axis=-1, keepdims=True) * (1.0 / depth)
    squares = jnp.zeros((2 * out_rows, HD), F32)
    for at in range(0, depth, HD):
        centered = mixed[:, pl.ds(at, HD)] - mean
        squares = squares + centered * centered
    scale = lax.rsqrt(jnp.sum(squares, axis=-1, keepdims=True) * (1.0 / depth) + EPS)
    velocity = bfin[...]
    for at in range(0, depth, chunk):
        cols = pl.ds(at, chunk)
        final_in = (mixed[:, cols] - mean) * scale
        final_in = jnp.concatenate(
            [
                final_in[:out_rows] * (1.0 + fmod[1:2, cols]) + fmod[0:1, cols],
                final_in[out_rows:] * (1.0 + fmod_in[1:2, cols]) + fmod_in[0:1, cols],
            ],
            axis=0,
        ).astype(BF)
        velocity = velocity + lax.dot_general(
            final_in, wfin[:, cols], (((1,), (1,)), ((), ())), preferred_element_type=F32
        )
    ch = velocity.shape[1]

    index = jnp.full((1, ch), step_index[0], jnp.int32).astype(F32)
    count = jnp.full((1, ch), step_count[0], jnp.int32).astype(F32)
    strength = jnp.full((1, ch), guidance[0], F32)
    sigma_prev = noise_level(index - 1.0, count)
    sigma_now = noise_level(index, count)
    sigma_next = noise_level(index + 1.0, count)
    step_now = log_ratio(sigma_next) - log_ratio(sigma_now)
    step_prev = log_ratio(sigma_now) - log_ratio(sigma_prev)
    ratio = step_prev / step_now
    ours, theirs = velocity[:out_rows], velocity[out_rows:]
    cond = jnp.where(c == 0, ours, theirs)
    uncond = jnp.where(c == 0, theirs, ours)
    guided = uncond + strength * (cond - uncond)
    denoised = lat[...] - sigma_now * guided
    blend = (1.0 + 0.5 / ratio) * denoised - 0.5 / ratio * prev[...]
    next_ref[...] = (
        sigma_next / sigma_now * lat[...] - (1.0 - sigma_next) * (jnp.exp(-step_now) - 1.0) * blend
    )
    den_ref[...] = denoised

    fresh_out.wait()
    for h in range(heads):
        for side in range(2):
            hop(side, 1, h).wait_send()

    def drain(stage, carry):
        for h in range(heads):
            for side in range(2):
                hop(side, stage, h).wait_send()
        return carry

    lax.fori_loop(2, last, drain, 0)
    for side in range(2):
        for h, kv in final_pieces[side]:
            hop(side, last, h, kv).wait_send()
    for h in range(heads):
        for f, k in peers8:
            a_copy(h, f, k).wait_send()
    for copy in (w1, w3, w2a, w2b, *d_out, *b_copies):
        copy.wait_send()


def hand_over(*refs):
    n = 3
    ins, outs, held, sems = refs[:n], refs[n : 2 * n], refs[2 * n : 3 * n], refs[3 * n :]
    reads = [pltpu.make_async_copy(a, b, sems[0].at[i]) for i, (a, b) in enumerate(zip(ins, held))]
    writes = [pltpu.make_async_copy(a, b, sems[1].at[i]) for i, (a, b) in enumerate(zip(held, outs))]
    for copy in reads:
        copy.start()
    for i in range(n):
        reads[i].wait()
        writes[i].start()
    for copy in writes:
        copy.wait()


def body(
    sizes,
    img_hidden, txt_hidden, modulation, w_qkv, q_gain, k_gain, w_out, b_out, stale_kv,
    final_mod, w_final, b_final, latent, prev_denoised, guidance, step_index, step_count,
):
    n_patch, n_head = sizes
    rows, depth = img_hidden.shape[1:]
    trows = txt_hidden.shape[1]
    kv_rows = rows + trows
    width = w_out.shape[0]
    heads = width // HD
    out_rows, ch = latent.shape
    last = n_patch // 2
    n_rows = n_patch * rows // GRID_W
    rowtab, coltab = rotation_tables(n_rows)
    any_spec = pl.BlockSpec(memory_space=pl.ANY)
    vmem = pl.BlockSpec(memory_space=pltpu.VMEM)
    dma = pltpu.SemaphoreType.DMA
    V = pltpu.VMEM
    outs = pl.pallas_call(
        functools.partial(kernel, sizes),
        out_shape=(
            jax.ShapeDtypeStruct((2, kv_rows, width), BF),
            jax.ShapeDtypeStruct((out_rows, ch), F32),
            jax.ShapeDtypeStruct((out_rows, ch), F32),
        ),
        in_specs=[any_spec] * 16 + [pl.BlockSpec(memory_space=pltpu.HBM)] * 3,
        out_specs=(any_spec, vmem, vmem),
        scratch_shapes=[
            V((heads, 2, kv_rows, HD), BF), V((rows, depth), BF), V((trows, depth), BF), V((3, 1, depth), F32),
            V((3, depth, width), BF), V((1, HD), F32), V((1, HD), F32), V((1, depth), F32),
            V((2, depth), F32), V((ch, depth), BF), V((1, ch), F32), V((out_rows, ch), F32),
            V((out_rows, ch), F32), V((3, n_rows, HD), F32), V((3, GRID_W, HD), F32),
            pltpu.SMEM((1,), F32), pltpu.SMEM((1,), jnp.int32), pltpu.SMEM((1,), jnp.int32),
            V((kv_rows, depth), BF), V((3, kv_rows, width), F32), V((3, kv_rows, HD), F32),
            V((2, kv_rows, width), BF), V((heads, HD, rows), BF), V((heads, 1, rows), F32),
            V((heads, 1, rows), F32), V((heads, HD, rows), F32),
            V((last, heads, 2, kv_rows, HD), BF), V((last - 1, heads, 2, kv_rows, HD), BF),
            V((2, heads, n_head, HD, depth // 2), BF),
            V((heads, 2, n_head, out_rows, HD), BF), V((heads, 2, out_rows, n_head * HD), BF),
            V((2 * out_rows, depth), F32), V((2 * out_rows, depth), F32),
            V((out_rows, depth), BF), V((1, depth), F32), V((2, depth), F32),
            dma((heads, 2)), dma((21,)), dma((1,)),
            dma((2, last, heads)), dma((2, last, heads)),
            dma((4,)), dma((4,)), dma((n_head - 1,)), dma((n_head - 1,)),
            dma((heads, 2, n_head)), dma((heads, 2, n_head)), dma((3,)), dma((3,)),
        ],
        compiler_params=pltpu.CompilerParams(
            collective_id=0, has_side_effects=True, vmem_limit_bytes=60 * 1024 * 1024
        ),
    )(
        img_hidden[0], txt_hidden[0], modulation.transpose(1, 0, 2), w_qkv.transpose(1, 0, 2),
        q_gain[None], k_gain[None], w_out.reshape(heads, HD, depth), b_out[None], stale_kv[0], final_mod[0], w_final.T,
        b_final[None], latent, prev_denoised, jnp.asarray(rowtab), jnp.asarray(coltab),
        guidance, step_index, step_count,
    )
    outs = pl.pallas_call(
        hand_over,
        out_shape=tuple(jax.ShapeDtypeStruct(o.shape, o.dtype) for o in outs),
        in_specs=[any_spec] * 3,
        out_specs=(any_spec,) * 3,
        scratch_shapes=[V(o.shape, o.dtype) for o in outs] + [dma((3,)), dma((3,))],
    )(*outs)
    return outs[0][None], outs[1], outs[2]


def solution(mesh):
    sizes = (mesh.shape["patch"], mesh.shape["head"])
    rows4 = P(("groups", "patch", "cfg", "head"), None)
    return jax.shard_map(
        functools.partial(body, sizes),
        mesh=mesh,
        in_specs=(
            P("cfg", ("groups", "patch"), None),
            P("cfg", ("groups", "patch"), None),
            P(("groups", "cfg"), None, None),
            P(None, None, "head"),
            P(),
            P(),
            P("head", None),
            P(),
            P("cfg", None, ("groups", "patch"), "head"),
            P(("groups", "cfg"), None, None),
            P(),
            P(),
            rows4,
            rows4,
            P("groups"),
            P(),
            P(),
        ),
        out_specs=(P("cfg", None, ("groups", "patch"), "head"), rows4, rows4),
        check_vma=False,
    )
```
